32 devices in a mesh: row: 4 (over y, x), col: 8 (over z, core).
Axes of the slice: x: 2, y: 2, z: 4, core: 2. Of those that a mesh axis runs over, the one named last changes fastest.
Arguments:
- pair: float32 [256, 256, 128], P('row', 'col'), may hold values from -6 to 6
- valid_length: int32 [1], replicated, may hold values from 64 to 255
- tri_in: bfloat16 [128, 512], replicated, may hold values from -0.5 to 0.5
- tri_gate: bfloat16 [128, 128], replicated, may hold values from -0.5 to 0.5
- tri_out: bfloat16 [128, 128], replicated, may hold values from -0.5 to 0.5
- att_in: bfloat16 [128, 512], replicated, may hold values from -16.9705627 to 16.9705627
- att_bias: bfloat16 [128, 4], replicated, may hold values from -0.5 to 0.5
- att_out: bfloat16 [128, 128], replicated, may hold values from -0.5 to 0.5
Outputs:
- pair_out: float32 [256, 256, 128], P('row', 'col')
The draws below stay inside these ranges and needn't reach their ends.
Inputs may be any that keep to these rules, and one draw needn't show every extreme that they name: Tokens at positions below valid_length[0] are real, the rest are padding.
All inputs are finite; a program needn't handle non-finite values.
Results may differ from the reference program's by a relative error of at most 0.025.
Values may be sent and summed in bfloat16 or wider, within the bound.
A program may use at most 128 MiB of HBM per device.

```python
import jax
import jax.numpy as jnp
from jax import lax

C = 128
CH = 128
H = 4
DH = 32
N = 256


def draw_att_in(key, part):
    raw = jax.random.truncated_normal(key, -4.0, 4.0, (C, 4 * C), jnp.float32) * C ** (-0.5)
    return raw.astype(jnp.bfloat16)


def shard_levels(stream_key, dims, shards, least, largest):
    factor_of, own = 1.0, jax.random.fold_in(stream_key, 6)
    for dim, shards_of in shards:
        heights = jnp.exp(jax.random.uniform(jax.random.fold_in(own, dim), (shards_of,), jnp.float32, least / len(shards), largest / len(shards)))
        factor_of = factor_of * jnp.repeat(heights, dims[dim] // shards_of).reshape([-1 if axis == dim else 1 for axis in range(len(dims))])
    return factor_of


def noise(key, extent, width, most, shards=(), held_as=jnp.bfloat16):
    array = width * jax.random.normal(key, extent, jnp.float32)
    if shards:
        array = array * shard_levels(key, extent, shards, -0.22, 0.18)
    return jnp.clip(array, -most, most).astype(held_as)


def setup_inputs(seed: int = 0) -> dict:
    splits = jax.random.split(jax.random.key(seed), 9)
    return {
        "pair": noise(splits[0], (N, N, C), 1.0, 6.0, ((0, 4), (1, 8)), jnp.float32),
        "valid_length": jax.random.randint(splits[1], (1,), N // 4, N).astype(jnp.int32),
        "tri_in": noise(splits[2], (C, 4 * CH), C ** -0.5, 0.5),
        "tri_gate": noise(splits[3], (C, C), C ** -0.5, 0.5),
        "tri_out": noise(splits[4], (CH, C), CH ** -0.5, 0.5),
        "att_in": draw_att_in(jax.random.fold_in(splits[8], 71), 0),
        "att_bias": noise(splits[6], (C, H), C ** -0.5, 0.5),
        "att_out": noise(splits[7], (C, C), C ** -0.5, 0.5),
    }


def layer_norm(values):
    center = values - lax.optimization_barrier(jnp.mean(values, axis=-1, keepdims=True))
    return center * lax.rsqrt(lax.optimization_barrier(jnp.mean(center * center, axis=-1, keepdims=True)) + 1e-05)

def reference(pair, valid_length, tri_in, tri_gate, tri_out, att_in, att_bias, att_out):
    tokens = jnp.arange(N).astype(jnp.int32)
    keep = (tokens < valid_length[0]).astype(jnp.float32)
    blocks = N // 8
    normed_pair = layer_norm(pair).astype(jnp.bfloat16)

    def edges(packed):
        rows, row_keep = packed
        projected = jnp.dot(rows, tri_in, preferred_element_type=jnp.float32)
        weight = (row_keep[:, None] * keep[None, :])[:, :, None]
        left = jax.nn.sigmoid(projected[..., :CH]) * projected[..., CH:2 * CH] * weight
        right = jax.nn.sigmoid(projected[..., 2 * CH:3 * CH]) * projected[..., 3 * CH:] * weight
        return (left.astype(jnp.bfloat16), right.astype(jnp.bfloat16))
    left_edges, right_edges = lax.map(edges, (normed_pair.reshape(blocks, 8, N, C), keep.reshape(blocks, 8)))
    left_edges = left_edges.reshape(N, N, CH)
    right_edges = right_edges.reshape(N, N, CH)
    products = jnp.einsum('ikc,jkc->ijc', left_edges.astype(jnp.float32), right_edges.astype(jnp.float32))
    normed_products = layer_norm(products).astype(jnp.bfloat16)
    update = jax.nn.sigmoid(jnp.dot(normed_pair, tri_gate, preferred_element_type=jnp.float32)) * jnp.dot(normed_products, tri_out, preferred_element_type=jnp.float32)
    middle = pair + update
    normed_mid = layer_norm(middle).astype(jnp.bfloat16)
    bias_all = jnp.dot(normed_mid, att_bias, preferred_element_type=jnp.float32).astype(jnp.bfloat16)
    bias_heads = jnp.transpose(bias_all.astype(jnp.float32), (2, 0, 1))
    mask_bias = jnp.where(tokens < valid_length[0], 0.0, -1000000000.0).astype(jnp.float32)

    def attend(packed):
        block_mid, block_norm = packed
        projected = jnp.dot(block_norm, att_in, preferred_element_type=jnp.float32)
        query = (projected[..., :C] * DH ** (-0.5)).astype(jnp.bfloat16).reshape(8, N, H, DH)
        keys = projected[..., C:2 * C].astype(jnp.bfloat16).reshape(8, N, H, DH)
        values = projected[..., 2 * C:3 * C].astype(jnp.bfloat16).reshape(8, N, H, DH)
        gate = jax.nn.sigmoid(projected[..., 3 * C:])
        scores = jnp.einsum('ijhd,ikhd->ihjk', query.astype(jnp.float32), keys.astype(jnp.float32))
        scores = scores + bias_heads[None] + mask_bias[None, None, None, :]
        weights = jax.nn.softmax(scores, axis=-1)
        attended = jnp.einsum('ihjk,ikhd->ijhd', weights, values.astype(jnp.float32)).reshape(8, N, C)
        gated = (gate * attended).astype(jnp.bfloat16)
        return block_mid + jnp.dot(gated, att_out, preferred_element_type=jnp.float32)
    result = lax.map(attend, (middle.reshape(blocks, 8, N, C), normed_mid.reshape(blocks, 8, N, C)))
    return result.reshape(N, N, C)
```

```python
import functools

import jax
import jax.numpy as jnp
from jax import lax
from jax.experimental import pallas as pl
from jax.experimental.pallas import tpu as pltpu
from jax.sharding import PartitionSpec as P

MESH = pl.DeviceIdType.MESH
F32 = jnp.float32
BF16 = jnp.bfloat16
scope = jax.named_scope


def norm(values, axis):
    center = values - jnp.mean(values, axis=axis, keepdims=True)
    return center * lax.rsqrt(jnp.mean(center * center, axis=axis, keepdims=True) + 1e-05)


def swap_groups(blocks, lane, group):
    count = len(blocks)
    width = count * group
    out = []
    for b in range(count):
        total = None
        for a in range(count):
            shift = (group * (a - b)) % width
            moved = blocks[a] if shift == 0 else pltpu.roll(blocks[a], shift, 1)
            total = moved if total is None else jnp.where(lane == a, moved, total)
        out.append(total)
    return out


def arrived(ref, sem):
    pltpu.make_async_copy(ref, ref, sem).wait()


def kernel(
    dims,
    valid_ref, pair_h, tri_in_h, tri_gate_h, tri_out_h, att_in_h, bias_w_h, att_out_h,
    out_ref,
    pair_ref, tri_in_ref, tri_gate_ref, tri_out_ref, att_in_ref, bias_w_ref, att_out_ref,
    normed_s, edge_f, left_send, right_send, left_recv, right_recv, left_s, right_s,
    prod_send, prod_recv, prod_f, tri_gate_s, mid_send, mid_recv, qkv_s, gate_s,
    bias_f, bias_recv, bias_full, gated_s, gated_recv,
    sem_in, send_l, recv_l, send_r, recv_r, send_p, recv_p, send_m, recv_m,
    send_b, recv_b, send_g, recv_g,
):
    nrow, ncol, rows_dev, cols_dev, width, heads, parts, halves = dims
    ndev = nrow * ncol
    total = ncol * cols_dev
    group = 128 // cols_dev
    tiles = rows_dev // group
    chans = width // ndev
    each = chans // parts
    per = rows_dev // ncol
    high = tiles // halves
    nz = ncol // 2
    head_size = width // heads
    my_row, my_col = lax.axis_index("row"), lax.axis_index("col")
    me = my_row * ncol + my_col
    core, my_z = lax.rem(my_col, 2), my_col // 2

    held = (pair_ref, tri_in_ref, tri_gate_ref, tri_out_ref, att_in_ref, bias_w_ref, att_out_ref)
    given = (pair_h, tri_in_h, tri_gate_h, tri_out_h, att_in_h, bias_w_h, att_out_h)
    loads = [pltpu.make_async_copy(g, v, sem_in.at[k]) for k, (g, v) in enumerate(zip(given, held))]
    for k in (0, 1, 2, 3, 5, 4, 6):
        loads[k].start()

    def other(step):
        peer = lax.rem(me + step, ndev)
        return peer, (peer // ncol, lax.rem(peer, ncol))

    def loop(count, act):
        def run(step, carry):
            act(step)
            return carry

        lax.fori_loop(1, count, run, 0)

    with scope("signal"):
        barrier = pltpu.get_barrier_semaphore()
        loop(
            ndev,
            lambda step: pl.semaphore_signal(
                barrier, inc=1, device_id=other(step)[1], device_id_type=MESH
            ),
        )
    with scope("inputs"):
        for k in (0, 1):
            loads[k].wait()
    valid = valid_ref[0]

    lanes = lax.broadcasted_iota(jnp.int32, (1, 128), 1)
    lane_col = my_col * cols_dev + lanes % cols_dev
    lane_row = my_row * rows_dev + (lanes // cols_dev) * tiles

    def edges(side):
        first = 2 * side * width
        for t in range(tiles):
            if side == 0:
                rows = jnp.concatenate([pair_ref[g * tiles + t] for g in range(group)], axis=0)
                normed_s[t] = norm(rows, 1).astype(BF16)
            proj = jnp.dot(
                normed_s[t], tri_in_ref[:, first : first + 2 * width], preferred_element_type=F32
            )
            keep = jnp.where((lane_row + t < valid) & (lane_col < valid), 1.0, 0.0)
            edge = jax.nn.sigmoid(proj[:, :width]) * proj[:, width:]
            edge_f[side, pl.ds(t, width, stride=tiles), :] = jnp.transpose(edge) * keep

    def pack(side, target):
        for c in range(chans):
            target[c] = edge_f[side, pl.ds(c * ndev * tiles, ndev * tiles), :].astype(BF16)

    def share(peer):
        return pl.ds(pl.multiple_of(peer * tiles, tiles), tiles)

    def remote(src, dst, send, recv, where):
        return pltpu.make_async_remote_copy(
            src_ref=src, dst_ref=dst, send_sem=send, recv_sem=recv, device_id=where, device_id_type=MESH
        )

    def left_copy(step):
        peer, where = other(step)
        return remote(left_send.at[:, share(peer), :], left_recv.at[me], send_l, recv_l, where)

    def right_copy(part, step):
        peer, where = other(step)
        some = pl.ds(part * each, each)
        return remote(
            right_send.at[some, share(peer), :], right_recv.at[part, me],
            send_r.at[part], recv_r.at[part], where,
        )

    with scope("edges0"):
        edges(0)
        pack(0, left_send)
    with scope("barrier"):
        pl.semaphore_wait(barrier, ndev - 1)
    with scope("sendl"):
        loop(ndev, lambda step: left_copy(step).start())
    with scope("edges1"):
        edges(1)
        pack(1, right_send)
    with scope("sendr"):
        for part in range(parts):
            loop(ndev, lambda step: right_copy(part, step).start())
    with scope("gate"):
        left_recv[me] = left_send[:, share(me), :]
        for part in range(parts):
            right_recv[part, me] = right_send[part * each : (part + 1) * each, share(me), :]
        for k in (2, 3, 5, 4, 6):
            loads[k].wait()
        for t in range(tiles):
            tri_gate_s[t] = jax.nn.sigmoid(
                jnp.dot(normed_s[t], tri_gate_ref[...], preferred_element_type=F32)
            )
    others = pl.ds(0, ndev - 1)
    with scope("waitl"):
        arrived(left_recv.at[others], recv_l)

    lane = lax.broadcasted_iota(jnp.int32, (tiles, 128), 1) // cols_dev

    def spread(load, operand):
        for r in range(nrow):
            for half in range(ncol // group):
                blocks = [load(r * ncol + half * group + a).astype(F32) for a in range(group)]
                for b, piece in enumerate(swap_groups(blocks, lane, cols_dev)):
                    operand[
                        pl.ds(r * rows_dev + b * tiles, tiles), pl.ds(half * 128, 128)
                    ] = piece.astype(BF16)

    def prod_copy(part, hh, step):
        peer, where = other(step)
        some = pl.ds(part * each * high, each * high)
        return remote(
            prod_send.at[peer, hh, some], prod_recv.at[hh, part, me],
            send_p.at[part, hh], recv_p.at[part, hh], where,
        )

    with scope("spreadl"):
        for c in range(chans):
            spread(lambda d: left_recv[d, c], left_s.at[c])
    for part in range(parts):
        with scope("waitr"):
            arrived(right_recv.at[part, others], recv_r.at[part])
        with scope("products"):
            for c in range(part * each, (part + 1) * each):
                spread(lambda d: right_recv[part, d, c - part * each], right_s.at[c])
                products = lax.dot_general(
                    left_s[c], right_s[c], (((1,), (1,)), ((), ())), preferred_element_type=F32
                )
                for r in range(nrow):
                    for half in range(ncol // group):
                        blocks = [
                            products[
                                r * rows_dev + a * tiles : r * rows_dev + (a + 1) * tiles,
                                half * 128 : (half + 1) * 128,
                            ]
                            for a in range(group)
                        ]
                        for b, piece in enumerate(swap_groups(blocks, lane, cols_dev)):
                            for hh in range(halves):
                                prod_send[r * ncol + half * group + b, hh, c * high : (c + 1) * high] = piece[
                                    hh * high : (hh + 1) * high
                                ].astype(BF16)
        with scope("sendp"):
            for hh in range(halves):
                loop(ndev, lambda step: prod_copy(part, hh, step).start())
                prod_recv[hh, part, me] = prod_send[me, hh, part * each * high : (part + 1) * each * high]

    def strip(peer):
        return pl.ds(pl.multiple_of(peer * cols_dev, cols_dev), cols_dev)

    def send_rows(t):
        i = t % per
        for g in range(group):
            turn = lax.rem(g + my_z, group)
            owner = turn * (tiles // per) + t // per

            @pl.when(owner != my_col)
            def _():
                remote(
                    mid_send.at[t, strip(turn), :], mid_recv.at[i, strip(my_col), :],
                    send_m, recv_m.at[i], (my_row, owner),
                ).start()

            @pl.when(owner == my_col)
            def _():
                mid_recv[i, strip(my_col), :] = mid_send[t, strip(turn), :]

    def bias_z(hh):
        def act(step):
            peer = lax.rem(my_z + step, nz)
            mine = bias_recv.at[core, hh, my_row, my_z]
            remote(mine, mine, send_b.at[0, hh], recv_b.at[0, hh], (my_row, 2 * peer + core)).start()

        loop(nz, act)

    def bias_row(hh):
        arrived(bias_recv.at[0, hh, 0, pl.ds(0, nz - 1)], recv_b.at[0, hh])

        def act(step):
            peer = lax.rem(my_row + step, nrow)
            mine = bias_recv.at[core, hh, my_row]
            remote(mine, mine, send_b.at[1, hh], recv_b.at[1, hh], (peer, my_col)).start()

        loop(nrow, act)

    def bias_hand(hh):
        mine = bias_recv.at[core, hh]
        return remote(mine, mine, send_b.at[2, hh], recv_b.at[2, hh], (my_row, my_col + 1 - 2 * core))

    def bias_core(hh):
        arrived(bias_recv.at[0, hh, pl.ds(0, nrow - 1)], recv_b.at[1, hh])
        bias_hand(hh).start()

    for hh in range(halves):
        with scope("waitp"):
            for part in range(parts):
                arrived(prod_recv.at[hh, part, others], recv_p.at[part, hh])
        with scope("unpack"):
            for part in range(parts):
                for d in range(ndev):
                    for c in range(each):
                        at = ((part * each + c) * ndev + d) * high
                        prod_f[at : at + high, :] = prod_recv[hh, part, d, c * high : (c + 1) * high].astype(F32)
        with scope("middle"):
            for tt in range(high):
                t = hh * high + tt
                prods = norm(prod_f[pl.ds(tt, width, stride=high), :], 0)
                prods = jnp.transpose(prods).astype(BF16)
                update = jnp.dot(prods, tri_out_ref[...], preferred_element_type=F32)
                rows = jnp.concatenate([pair_ref[g * tiles + t] for g in range(group)], axis=0)
                middle = rows + tri_gate_s[t] * update
                normed_mid = norm(middle, 1).astype(BF16)
                for g in range(group):
                    out_ref[g * tiles + t] = middle[g * cols_dev : (g + 1) * cols_dev]
                mid_send[t] = normed_mid
                send_rows(t)
                own = lax.dot_general(
                    bias_w_ref[...], normed_mid, (((1,), (1,)), ((), ())), preferred_element_type=F32
                )
                for h in range(heads):
                    bias_f[pl.ds(h * high + tt, 1), :] = own[h : h + 1]
        with scope("bias_z"):
            bias_recv[core, hh, my_row, my_z] = bias_f[...].astype(BF16)
            bias_z(hh)
            if hh > 0:
                bias_row(hh - 1)

    def take(i):
        arrived(mid_recv.at[i, pl.ds(0, (ncol - 1) * cols_dev), :], recv_m.at[i])

    tokens = lax.broadcasted_iota(jnp.int32, (1, total), 1)
    mask = jnp.where(tokens < valid, 0.0, -1000000000.0)
    narrow = lax.broadcasted_iota(jnp.int32, (high, 128), 1) // cols_dev

    def assemble(hh):
        arrived(bias_recv.at[0, hh], recv_b.at[2, hh])
        for h in range(heads):
            for r in range(nrow):
                for half in range(ncol // group):
                    blocks = []
                    for a in range(group):
                        c = half * group + a
                        blocks.append(
                            bias_recv[c % 2, hh, r, c // 2, h * high : (h + 1) * high, :].astype(F32)
                        )
                    for b, piece in enumerate(swap_groups(blocks, narrow, cols_dev)):
                        bias_full[
                            h, pl.ds(r * rows_dev + b * tiles + hh * high, high), pl.ds(half * 128, 128)
                        ] = piece + mask[:, half * 128 : (half + 1) * 128]

    def project(i):
        with scope("take"):
            take(i)
        with scope("project"):
            proj = jnp.dot(mid_recv[i], att_in_ref[...], preferred_element_type=F32)
            qkv_s[i, :, :width] = (proj[:, :width] * head_size ** (-0.5)).astype(BF16)
            qkv_s[i, :, width : 3 * width] = proj[:, width : 3 * width].astype(BF16)
            gate_s[i] = jax.nn.sigmoid(proj[:, 3 * width :])

    ready = per // 2
    for i in range(ready):
        project(i)
    for hh in range(halves - 1):
        with scope("bias_core"):
            bias_core(hh)
    with scope("bias_row"):
        bias_row(halves - 1)
    for hh in range(halves - 1):
        with scope("assemble"):
            assemble(hh)
    with scope("bias_core"):
        bias_core(halves - 1)
    with scope("assemble"):
        assemble(halves - 1)

    block = 128
    head = lax.broadcasted_iota(jnp.int32, (block, width), 1) // head_size

    def home_copy(i, step):
        peer = lax.rem(my_col + step, ncol)
        return remote(
            gated_s.at[i, strip(peer), :], gated_recv.at[i, strip(my_col), :],
            send_g, recv_g.at[i], (my_row, peer),
        )

    def attend(i):
        keys = qkv_s[i, :, width : 2 * width]
        values = jnp.concatenate(
            [qkv_s[i, :, 2 * width : 3 * width], jnp.ones((total, width), BF16)], axis=1
        )
        for first in range(0, total, block):
            query = qkv_s[i, first : first + block, :width]
            top = jnp.zeros((block, width), F32)
            bottom = jnp.ones((block, width), F32)
            for h in range(heads):
                scores = lax.dot_general(
                    jnp.where(head == h, query, jnp.zeros_like(query)), keys,
                    (((1,), (1,)), ((), ())), preferred_element_type=F32,
                )
                scores = scores + bias_full[h, first : first + block, :]
                expo = jnp.exp(scores - jnp.max(scores, axis=1, keepdims=True)).astype(BF16)
                both = jnp.dot(expo, values, preferred_element_type=F32)
                top = jnp.where(head == h, both[:, :width], top)
                bottom = jnp.where(head == h, both[:, width:], bottom)
            gated_s[i, first : first + block, :] = (
                gate_s[i, first : first + block, :] * top / bottom
            ).astype(BF16)
        for step in range(1, ncol):
            home_copy(i, step).start()
        gated_recv[i, strip(my_col), :] = gated_s[i, strip(my_col), :]

    with scope("attend0"):
        lax.fori_loop(0, ready, lambda i, carry: (attend(i), carry)[1], 0)

    def both(i, carry):
        project(i)
        attend(i)
        return carry

    with scope("attend1"):
        lax.fori_loop(ready, per, both, 0)

    def finish(i, carry):
        with scope("waitg"):
            arrived(gated_recv.at[i, pl.ds(0, (ncol - 1) * cols_dev), :], recv_g.at[i])
        added = jnp.dot(gated_recv[i], att_out_ref[...], preferred_element_type=F32)
        for q in range(ncol):
            out_ref[q * per + i] += added[q * cols_dev : (q + 1) * cols_dev]
        return carry

    with scope("finish"):
        lax.fori_loop(0, per, finish, 0)
    with scope("drain"):
        arrived(left_recv.at[others], send_l)
        for part in range(parts):
            arrived(right_recv.at[part, others], send_r.at[part])
            for hh in range(halves):
                arrived(prod_recv.at[hh, part, others], send_p.at[part, hh])
        for i in range(per):
            arrived(mid_recv.at[i, pl.ds(0, (ncol - 1) * cols_dev), :], send_m)
            arrived(mid_recv.at[i, pl.ds(0, (ncol - 1) * cols_dev), :], send_g)
        for hh in range(halves):
            arrived(bias_recv.at[0, hh, 0, pl.ds(0, nz - 1)], send_b.at[0, hh])
            arrived(bias_recv.at[0, hh, pl.ds(0, nrow - 1)], send_b.at[1, hh])
            arrived(bias_recv.at[0, hh], send_b.at[2, hh])


def per_device(pair, valid_length, tri_in, tri_gate, tri_out, att_in, att_bias, att_out):
    rows_dev, cols_dev, width = pair.shape
    heads = att_bias.shape[1]
    nrow, ncol = lax.axis_size("row"), lax.axis_size("col")
    ndev = nrow * ncol
    total = ncol * cols_dev
    tiles = rows_dev // (128 // cols_dev)
    chans = width // ndev
    parts = 2 if chans % 2 == 0 else 1
    each = chans // parts
    per = rows_dev // ncol
    halves = 2 if tiles % 16 == 0 and (tiles // 2) % per == 0 else 1
    high = tiles // halves
    hbm = pl.BlockSpec(memory_space=pltpu.HBM)
    vmem = pl.BlockSpec(memory_space=pltpu.VMEM)
    held = lambda dtype, *shape: pltpu.VMEM(shape, dtype)
    sem = lambda *shape: pltpu.SemaphoreType.DMA(shape) if shape else pltpu.SemaphoreType.DMA
    bias_w = att_bias.T
    args = [pltpu.with_memory_space_constraint(a, pltpu.HBM) for a in (pair, tri_in, tri_gate, tri_out, att_in, bias_w, att_out)]
    return pl.pallas_call(
        functools.partial(kernel, (nrow, ncol, rows_dev, cols_dev, width, heads, parts, halves)),
        out_shape=jax.ShapeDtypeStruct((rows_dev, cols_dev, width), F32),
        in_specs=[pl.BlockSpec(memory_space=pltpu.SMEM)] + [hbm] * 7,
        out_specs=vmem,
        scratch_shapes=[
            *[held(a.dtype, *a.shape) for a in args],
            held(BF16, tiles, 128, width),
            held(F32, 2, width * tiles, 128),
            held(BF16, chans, ndev * tiles, 128),
            held(BF16, chans, ndev * tiles, 128),
            held(BF16, ndev, chans, tiles, 128),
            held(BF16, parts, ndev, each, tiles, 128),
            held(BF16, chans, total, total),
            held(BF16, chans, total, total),
            held(BF16, ndev, halves, chans * high, 128),
            held(BF16, halves, parts, ndev, each * high, 128),
            held(F32, width * high, 128),
            held(F32, tiles, 128, width),
            held(BF16, tiles, 128, width),
            held(BF16, per, total, width),
            held(BF16, per, total, 3 * width),
            held(F32, per, total, width),
            held(F32, heads * high, 128),
            held(BF16, 2, halves, nrow, ncol // 2, heads * high, 128),
            held(F32, heads, total, total),
            held(BF16, per, total, width),
            held(BF16, per, total, width),
            sem(7), sem(), sem(), sem(parts), sem(parts), sem(parts, halves), sem(parts, halves),
            sem(), sem(per), sem(3, halves), sem(3, halves), sem(), sem(per),
        ],
        compiler_params=pltpu.CompilerParams(
            collective_id=0, has_side_effects=True, vmem_limit_bytes=40 * 1024 * 1024
        ),
    )(valid_length, *args)


def solution(mesh):
    placed = (P("row", "col", None), P(), P(), P(), P(), P(), P(), P())
    return jax.shard_map(
        per_device, mesh=mesh, in_specs=placed, out_specs=P("row", "col", None), check_vma=False
    )
```

```python
import functools

import jax
import jax.numpy as jnp
from jax import lax
from jax.experimental import pallas as pl
from jax.experimental.pallas import tpu as pltpu
from jax.sharding import PartitionSpec as P

MESH = pl.DeviceIdType.MESH
F32 = jnp.float32
BF16 = jnp.bfloat16
scope = jax.named_scope


def norm(values, axis):
    center = values - jnp.mean(values, axis=axis, keepdims=True)
    return center * lax.rsqrt(jnp.mean(center * center, axis=axis, keepdims=True) + 1e-05)


def swap_groups(blocks, lane, group):
    count = len(blocks)
    width = count * group
    out = []
    for b in range(count):
        total = None
        for a in range(count):
            shift = (group * (a - b)) % width
            moved = blocks[a] if shift == 0 else pltpu.roll(blocks[a], shift, 1)
            total = moved if total is None else jnp.where(lane == a, moved, total)
        out.append(total)
    return out


def arrived(ref, sem):
    pltpu.make_async_copy(ref, ref, sem).wait()


def kernel(
    dims,
    valid_ref, pair_h, tri_in_h, tri_gate_h, tri_out_h, att_in_h, bias_w_h, att_out_h,
    out_ref,
    pair_ref, tri_in_ref, tri_gate_ref, tri_out_ref, att_in_ref, bias_w_ref, att_out_ref,
    normed_s, edge_f, left_send, right_send, left_recv, right_recv, left_s, right_s,
    prod_send, prod_recv, prod_f, tri_gate_s, pair_s, middle_s, tri_out_s, mid_send, mid_recv, qkv_s, gate_s,
    bias_f, bias_recv, bias_full, gated_s, gated_recv,
    sem_in, send_l, recv_l, send_r, recv_r, send_p, recv_p, send_m, recv_m,
    send_b, recv_b, send_g, recv_g,
):
    nrow, ncol, rows_dev, cols_dev, width, heads, parts, halves = dims
    ndev = nrow * ncol
    total = ncol * cols_dev
    group = 128 // cols_dev
    tiles = rows_dev // group
    chans = width // ndev
    each = chans // parts
    per = rows_dev // ncol
    high = tiles // halves
    nz = ncol // 2
    head_size = width // heads
    my_row, my_col = lax.axis_index("row"), lax.axis_index("col")
    me = my_row * ncol + my_col
    core, my_z = lax.rem(my_col, 2), my_col // 2

    held = (pair_ref, tri_in_ref, tri_gate_ref, tri_out_ref, att_in_ref, bias_w_ref, att_out_ref)
    given = (pair_h, tri_in_h, tri_gate_h, tri_out_h, att_in_h, bias_w_h, att_out_h)
    loads = [pltpu.make_async_copy(g, v, sem_in.at[k]) for k, (g, v) in enumerate(zip(given, held))]
    for k in (0, 1, 2, 3, 5, 4, 6):
        loads[k].start()

    def other(step):
        peer = lax.rem(me + step, ndev)
        return peer, (peer // ncol, lax.rem(peer, ncol))

    def loop(count, act):
        def run(step, carry):
            act(step)
            return carry

        lax.fori_loop(1, count, run, 0)

    with scope("signal"):
        barrier = pltpu.get_barrier_semaphore()
        loop(
            ndev,
            lambda step: pl.semaphore_signal(
                barrier, inc=1, device_id=other(step)[1], device_id_type=MESH
            ),
        )
    with scope("inputs"):
        for k in (0, 1):
            loads[k].wait()
    valid = valid_ref[0]

    lanes = lax.broadcasted_iota(jnp.int32, (1, 128), 1)
    lane_col = my_col * cols_dev + lanes % cols_dev
    lane_row = my_row * rows_dev + (lanes // cols_dev) * tiles

    def edge(side, t):
        first = 2 * side * width
        if side == 0:
            rows = jnp.concatenate([pair_ref[g * tiles + t] for g in range(group)], axis=0)
            normed_s[t] = norm(rows, 1).astype(BF16)
        proj = jnp.dot(
            normed_s[t], tri_in_ref[:, first : first + 2 * width], preferred_element_type=F32
        )
        keep = jnp.where((lane_row + t < valid) & (lane_col < valid), 1.0, 0.0)
        return jnp.transpose(jax.nn.sigmoid(proj[:, :width]) * proj[:, width:]) * keep

    def left_edges(hh):
        for tt in range(high):
            edge_f[0, pl.ds(hh * width * high + tt, width, stride=high), :] = edge(0, hh * high + tt)
        for d in range(ndev):
            for c in range(chans):
                at = hh * width * high + (c * ndev + d) * high
                left_send[hh, d, c * high : (c + 1) * high] = edge_f[0, at : at + high, :].astype(BF16)

    def right_edges():
        for t in range(tiles):
            edge_f[1, pl.ds(t, width, stride=tiles), :] = edge(1, t)
        for c in range(chans):
            right_send[c] = edge_f[1, pl.ds(c * ndev * tiles, ndev * tiles), :].astype(BF16)

    def share(peer):
        return pl.ds(pl.multiple_of(peer * tiles, tiles), tiles)

    def remote(src, dst, send, recv, where):
        return pltpu.make_async_remote_copy(
            src_ref=src, dst_ref=dst, send_sem=send, recv_sem=recv, device_id=where, device_id_type=MESH
        )

    def left_copy(hh, step):
        peer, where = other(step)
        return remote(left_send.at[hh, peer], left_recv.at[hh, me], send_l.at[hh], recv_l.at[hh], where)

    def right_copy(part, step):
        peer, where = other(step)
        some = pl.ds(part * each, each)
        return remote(
            right_send.at[some, share(peer), :], right_recv.at[part, me],
            send_r.at[part], recv_r.at[part], where,
        )

    for hh in range(halves):
        with scope("edges0"):
            left_edges(hh)
        if hh == 0:
            with scope("barrier"):
                pl.semaphore_wait(barrier, ndev - 1)
        with scope("sendl"):
            loop(ndev, lambda step: left_copy(hh, step).start())
            left_recv[hh, me] = left_send[hh, me]
    with scope("edges1"):
        right_edges()
    with scope("sendr"):
        for part in range(parts):
            loop(ndev, lambda step: right_copy(part, step).start())
            right_recv[part, me] = right_send[part * each : (part + 1) * each, share(me), :]
    with scope("gate"):
        for k in (2, 3, 5, 4, 6):
            loads[k].wait()
        tri_out_s[...] = jnp.transpose(tri_out_ref[...].astype(F32)).astype(BF16)
        for t in range(tiles):
            tri_gate_s[t] = jax.nn.sigmoid(
                lax.dot_general(
                    tri_gate_ref[...], normed_s[t], (((0,), (1,)), ((), ())), preferred_element_type=F32
                )
            )
            rows = jnp.concatenate([pair_ref[g * tiles + t] for g in range(group)], axis=0)
            pair_s[t] = jnp.transpose(rows)
    others = pl.ds(0, ndev - 1)
    with scope("waitl"):
        for hh in range(halves):
            arrived(left_recv.at[hh, others], recv_l.at[hh])

    lane = lax.broadcasted_iota(jnp.int32, (tiles, 128), 1) // cols_dev

    def spread(load, operand):
        for r in range(nrow):
            for half in range(ncol // group):
                blocks = [load(r * ncol + half * group + a) for a in range(group)]
                for b, piece in enumerate(swap_groups(blocks, lane, cols_dev)):
                    operand[
                        pl.ds(r * rows_dev + b * tiles, tiles), pl.ds(half * 128, 128)
                    ] = piece.astype(BF16)

    def prod_copy(part, hh, step):
        peer, where = other(step)
        some = pl.ds(part * each * high, each * high)
        return remote(
            prod_send.at[peer, hh, some], prod_recv.at[hh, part, me],
            send_p.at[part, hh], recv_p.at[part, hh], where,
        )

    with scope("spreadl"):
        for c in range(chans):
            spread(
                lambda d: jnp.concatenate(
                    [left_recv[hh, d, c * high : (c + 1) * high].astype(F32) for hh in range(halves)], axis=0
                ),
                left_s.at[c],
            )
    for part in range(parts):
        with scope("waitr"):
            arrived(right_recv.at[part, others], recv_r.at[part])
        with scope("products"):
            for c in range(part * each, (part + 1) * each):
                spread(lambda d: right_recv[part, d, c - part * each].astype(F32), right_s.at[c])
                products = lax.dot_general(
                    left_s[c], right_s[c], (((1,), (1,)), ((), ())), preferred_element_type=F32
                )
                for r in range(nrow):
                    for half in range(ncol // group):
                        blocks = [
                            products[
                                r * rows_dev + a * tiles : r * rows_dev + (a + 1) * tiles,
                                half * 128 : (half + 1) * 128,
                            ]
                            for a in range(group)
                        ]
                        for b, piece in enumerate(swap_groups(blocks, lane, cols_dev)):
                            for hh in range(halves):
                                prod_send[r * ncol + half * group + b, hh, c * high : (c + 1) * high] = piece[
                                    hh * high : (hh + 1) * high
                                ].astype(BF16)
        with scope("sendp"):
            for hh in range(halves):
                loop(ndev, lambda step: prod_copy(part, hh, step).start())
                prod_recv[hh, part, me] = prod_send[me, hh, part * each * high : (part + 1) * each * high]

    def strip(peer):
        return pl.ds(pl.multiple_of(peer * cols_dev, cols_dev), cols_dev)

    def send_rows(t):
        i = t % per
        for g in range(group):
            turn = lax.rem(g + my_z, group)
            owner = turn * (tiles // per) + t // per

            @pl.when(owner != my_col)
            def _():
                remote(
                    mid_send.at[t, strip(turn), :], mid_recv.at[i, strip(my_col), :],
                    send_m, recv_m.at[i], (my_row, owner),
                ).start()

            @pl.when(owner == my_col)
            def _():
                mid_recv[i, strip(my_col), :] = mid_send[t, strip(turn), :]

    def bias_z(hh):
        def act(step):
            peer = lax.rem(my_z + step, nz)
            mine = bias_recv.at[core, hh, my_row, my_z]
            remote(mine, mine, send_b.at[0, hh], recv_b.at[0, hh], (my_row, 2 * peer + core)).start()

        loop(nz, act)

    def bias_row(hh):
        arrived(bias_recv.at[0, hh, 0, pl.ds(0, nz - 1)], recv_b.at[0, hh])

        def act(step):
            peer = lax.rem(my_row + step, nrow)
            mine = bias_recv.at[core, hh, my_row]
            remote(mine, mine, send_b.at[1, hh], recv_b.at[1, hh], (peer, my_col)).start()

        loop(nrow, act)

    def bias_hand(hh):
        mine = bias_recv.at[core, hh]
        return remote(mine, mine, send_b.at[2, hh], recv_b.at[2, hh], (my_row, my_col + 1 - 2 * core))

    def bias_core(hh):
        arrived(bias_recv.at[0, hh, pl.ds(0, nrow - 1)], recv_b.at[1, hh])
        bias_hand(hh).start()

    for hh in range(halves):
        with scope("waitp"):
            for part in range(parts):
                arrived(prod_recv.at[hh, part, others], recv_p.at[part, hh])
        with scope("unpack"):
            for part in range(parts):
                for d in range(ndev):
                    for c in range(each):
                        at = ((part * each + c) * ndev + d) * high
                        prod_f[at : at + high, :] = prod_recv[hh, part, d, c * high : (c + 1) * high].astype(F32)
        with scope("middle"):
            for tt in range(high):
                t = hh * high + tt
                prods = norm(prod_f[pl.ds(tt, width, stride=high), :], 0).astype(BF16)
                update = jnp.dot(tri_out_s[...], prods, preferred_element_type=F32)
                middle = pair_s[t] + tri_gate_s[t] * update
                middle_s[t] = middle
                normed_mid = norm(middle, 0)
                own = jnp.dot(bias_w_ref[...], normed_mid.astype(BF16), preferred_element_type=F32)
                for h in range(heads):
                    bias_f[pl.ds(h * high + tt, 1), :] = own[h : h + 1]
                mid_send[t] = jnp.transpose(normed_mid).astype(BF16)
        with scope("bias_z"):
            bias_recv[core, hh, my_row, my_z] = bias_f[...].astype(BF16)
            bias_z(hh)
        with scope("send_rows"):
            early = range(high // 2) if hh == 0 and halves > 1 else range(high)
            if hh > 0:
                for tt in range(high // 2 if hh == 1 else high, high):
                    send_rows((hh - 1) * high + tt)
            for tt in early:
                send_rows(hh * high + tt)

    def take(i):
        arrived(mid_recv.at[i, pl.ds(0, (ncol - 1) * cols_dev), :], recv_m.at[i])

    tokens = lax.broadcasted_iota(jnp.int32, (1, total), 1)
    mask = jnp.where(tokens < valid, 0.0, -1000000000.0)
    narrow = lax.broadcasted_iota(jnp.int32, (high, 128), 1) // cols_dev

    def assemble(hh):
        arrived(bias_recv.at[0, hh], recv_b.at[2, hh])
        for h in range(heads):
            for r in range(nrow):
                for half in range(ncol // group):
                    blocks = []
                    for a in range(group):
                        c = half * group + a
                        blocks.append(
                            bias_recv[c % 2, hh, r, c // 2, h * high : (h + 1) * high, :].astype(F32)
                        )
                    for b, piece in enumerate(swap_groups(blocks, narrow, cols_dev)):
                        bias_full[
                            h, pl.ds(r * rows_dev + b * tiles + hh * high, high), pl.ds(half * 128, 128)
                        ] = piece + mask[:, half * 128 : (half + 1) * 128]

    def project(i):
        with scope("take"):
            take(i)
        with scope("project"):
            proj = jnp.dot(mid_recv[i], att_in_ref[...], preferred_element_type=F32)
            qkv_s[i, :, :width] = (proj[:, :width] * head_size ** (-0.5)).astype(BF16)
            qkv_s[i, :, width : 3 * width] = proj[:, width : 3 * width].astype(BF16)
            gate_s[i] = jax.nn.sigmoid(proj[:, 3 * width :])

    with scope("keep_middle"):
        for t in range(tiles):
            middle = jnp.transpose(middle_s[t])
            for g in range(group):
                out_ref[g * tiles + t] = middle[g * cols_dev : (g + 1) * cols_dev]
    for hh in range(halves):
        with scope("bias_row"):
            bias_row(hh)
    for hh in range(halves):
        with scope("bias_core"):
            bias_core(hh)
    ready = per // 2
    for i in range(ready):
        project(i)
    for hh in range(halves):
        with scope("assemble"):
            assemble(hh)

    block = 128
    head = lax.broadcasted_iota(jnp.int32, (block, width), 1) // head_size

    def home_copy(i, step):
        peer = lax.rem(my_col + step, ncol)
        return remote(
            gated_s.at[i, strip(peer), :], gated_recv.at[i, strip(my_col), :],
            send_g, recv_g.at[i], (my_row, peer),
        )

    def attend(i):
        keys = qkv_s[i, :, width : 2 * width]
        values = jnp.concatenate(
            [qkv_s[i, :, 2 * width : 3 * width], jnp.ones((total, width), BF16)], axis=1
        )
        for first in range(0, total, block):
            query = qkv_s[i, first : first + block, :width]
            top = jnp.zeros((block, width), F32)
            bottom = jnp.ones((block, width), F32)
            for h in range(heads):
                scores = lax.dot_general(
                    jnp.where(head == h, query, jnp.zeros_like(query)), keys,
                    (((1,), (1,)), ((), ())), preferred_element_type=F32,
                )
                scores = scores + bias_full[h, first : first + block, :]
                expo = jnp.exp(scores - jnp.max(scores, axis=1, keepdims=True)).astype(BF16)
                both = jnp.dot(expo, values, preferred_element_type=F32)
                top = jnp.where(head == h, both[:, :width], top)
                bottom = jnp.where(head == h, both[:, width:], bottom)
            gated_s[i, first : first + block, :] = (
                gate_s[i, first : first + block, :] * top / bottom
            ).astype(BF16)
        for step in range(1, ncol):
            home_copy(i, step).start()
        gated_recv[i, strip(my_col), :] = gated_s[i, strip(my_col), :]

    with scope("attend0"):
        lax.fori_loop(0, ready, lambda i, carry: (attend(i), carry)[1], 0)

    def both(i, carry):
        project(i)
        attend(i)
        return carry

    with scope("attend1"):
        lax.fori_loop(ready, per, both, 0)

    def finish(i, carry):
        with scope("waitg"):
            arrived(gated_recv.at[i, pl.ds(0, (ncol - 1) * cols_dev), :], recv_g.at[i])
        added = jnp.dot(gated_recv[i], att_out_ref[...], preferred_element_type=F32)
        for q in range(ncol):
            out_ref[q * per + i] += added[q * cols_dev : (q + 1) * cols_dev]
        return carry

    with scope("finish"):
        lax.fori_loop(0, per, finish, 0)
    with scope("drain"):
        for hh in range(halves):
            arrived(left_recv.at[hh, others], send_l.at[hh])
        for part in range(parts):
            arrived(right_recv.at[part, others], send_r.at[part])
            for hh in range(halves):
                arrived(prod_recv.at[hh, part, others], send_p.at[part, hh])
        for i in range(per):
            arrived(mid_recv.at[i, pl.ds(0, (ncol - 1) * cols_dev), :], send_m)
            arrived(mid_recv.at[i, pl.ds(0, (ncol - 1) * cols_dev), :], send_g)
        for hh in range(halves):
            arrived(bias_recv.at[0, hh, 0, pl.ds(0, nz - 1)], send_b.at[0, hh])
            arrived(bias_recv.at[0, hh, pl.ds(0, nrow - 1)], send_b.at[1, hh])
            arrived(bias_recv.at[0, hh], send_b.at[2, hh])


def per_device(pair, valid_length, tri_in, tri_gate, tri_out, att_in, att_bias, att_out):
    rows_dev, cols_dev, width = pair.shape
    heads = att_bias.shape[1]
    nrow, ncol = lax.axis_size("row"), lax.axis_size("col")
    ndev = nrow * ncol
    total = ncol * cols_dev
    tiles = rows_dev // (128 // cols_dev)
    chans = width // ndev
    parts = 2 if chans % 2 == 0 else 1
    each = chans // parts
    per = rows_dev // ncol
    halves = 2 if tiles % 16 == 0 and (tiles // 2) % per == 0 else 1
    high = tiles // halves
    hbm = pl.BlockSpec(memory_space=pltpu.HBM)
    vmem = pl.BlockSpec(memory_space=pltpu.VMEM)
    held = lambda dtype, *shape: pltpu.VMEM(shape, dtype)
    sem = lambda *shape: pltpu.SemaphoreType.DMA(shape) if shape else pltpu.SemaphoreType.DMA
    bias_w = att_bias.T
    args = [pltpu.with_memory_space_constraint(a, pltpu.HBM) for a in (pair, tri_in, tri_gate, tri_out, att_in, bias_w, att_out)]
    return pl.pallas_call(
        functools.partial(kernel, (nrow, ncol, rows_dev, cols_dev, width, heads, parts, halves)),
        out_shape=jax.ShapeDtypeStruct((rows_dev, cols_dev, width), F32),
        in_specs=[pl.BlockSpec(memory_space=pltpu.SMEM)] + [hbm] * 7,
        out_specs=vmem,
        scratch_shapes=[
            *[held(a.dtype, *a.shape) for a in args],
            held(BF16, tiles, 128, width),
            held(F32, 2, width * tiles, 128),
            held(BF16, halves, ndev, chans * high, 128),
            held(BF16, chans, ndev * tiles, 128),
            held(BF16, halves, ndev, chans * high, 128),
            held(BF16, parts, ndev, each, tiles, 128),
            held(BF16, chans, total, total),
            held(BF16, chans, total, total),
            held(BF16, ndev, halves, chans * high, 128),
            held(BF16, halves, parts, ndev, each * high, 128),
            held(F32, width * high, 128),
            held(F32, tiles, width, 128),
            held(F32, tiles, width, 128),
            held(F32, tiles, width, 128),
            held(BF16, width, width),
            held(BF16, tiles, 128, width),
            held(BF16, per, total, width),
            held(BF16, per, total, 3 * width),
            held(F32, per, total, width),
            held(F32, heads * high, 128),
            held(BF16, 2, halves, nrow, ncol // 2, heads * high, 128),
            held(F32, heads, total, total),
            held(BF16, per, total, width),
            held(BF16, per, total, width),
            sem(7), sem(halves), sem(halves), sem(parts), sem(parts), sem(parts, halves), sem(parts, halves),
            sem(), sem(per), sem(3, halves), sem(3, halves), sem(), sem(per),
        ],
        compiler_params=pltpu.CompilerParams(
            collective_id=0, has_side_effects=True, vmem_limit_bytes=40 * 1024 * 1024
        ),
    )(valid_length, *args)


def solution(mesh):
    placed = (P("row", "col", None), P(), P(), P(), P(), P(), P(), P())
    return jax.shard_map(
        per_device, mesh=mesh, in_specs=placed, out_specs=P("row", "col", None), check_vma=False
    )
```

```python
import functools

import jax
import jax.numpy as jnp
from jax import lax
from jax.experimental import pallas as pl
from jax.experimental.pallas import tpu as pltpu
from jax.sharding import PartitionSpec as P

MESH = pl.DeviceIdType.MESH
F32 = jnp.float32
BF16 = jnp.bfloat16
scope = jax.named_scope


def norm(values, axis):
    center = values - jnp.mean(values, axis=axis, keepdims=True)
    return center * lax.rsqrt(jnp.mean(center * center, axis=axis, keepdims=True) + 1e-05)


def swap_groups(blocks, lane, group):
    count = len(blocks)
    width = count * group
    out = []
    for b in range(count):
        total = None
        for a in range(count):
            shift = (group * (a - b)) % width
            moved = blocks[a] if shift == 0 else pltpu.roll(blocks[a], shift, 1)
            total = moved if total is None else jnp.where(lane == a, moved, total)
        out.append(total)
    return out


def arrived(ref, sem):
    pltpu.make_async_copy(ref, ref, sem).wait()


def kernel(
    dims,
    valid_ref, pair_h, tri_in_h, tri_gate_h, tri_out_h, att_in_h, bias_w_h, att_out_h,
    out_ref,
    pair_ref, tri_in_ref, tri_gate_ref, tri_out_ref, att_in_ref, bias_w_ref, att_out_ref,
    normed_s, edge_f, left_send, right_send, left_recv, right_recv, left_s, right_s,
    prod_send, prod_recv, prod_f, tri_gate_s, pair_s, middle_s, tri_out_s, mid_send, mid_recv, kv_s, query_s, gate_s,
    bias_f, bias_recv, bias_full, gated_s, gated_recv,
    sem_in, send_l, recv_l, send_r, recv_r, send_p, recv_p, send_m, recv_m,
    send_b, recv_z, recv_b, send_g, recv_g,
):
    nrow, ncol, rows_dev, cols_dev, width, heads, parts, halves = dims
    ndev = nrow * ncol
    total = ncol * cols_dev
    group = 128 // cols_dev
    tiles = rows_dev // group
    chans = width // ndev
    each = chans // parts
    per = rows_dev // ncol
    span = tiles // per
    high = tiles // halves
    nz = ncol // 2
    head_size = width // heads
    my_row, my_col = lax.axis_index("row"), lax.axis_index("col")
    me = my_row * ncol + my_col
    core, my_z = lax.rem(my_col, 2), my_col // 2

    held = (pair_ref, tri_in_ref, tri_gate_ref, tri_out_ref, att_in_ref, bias_w_ref, att_out_ref)
    given = (pair_h, tri_in_h, tri_gate_h, tri_out_h, att_in_h, bias_w_h, att_out_h)
    loads = [pltpu.make_async_copy(g, v, sem_in.at[k]) for k, (g, v) in enumerate(zip(given, held))]
    for k in (0, 1, 2, 3, 5, 4, 6):
        loads[k].start()

    def other(step):
        peer = lax.rem(me + step, ndev)
        return peer, (peer // ncol, lax.rem(peer, ncol))

    def loop(count, act):
        def run(step, carry):
            act(step)
            return carry

        lax.fori_loop(1, count, run, 0)

    with scope("signal"):
        barrier = pltpu.get_barrier_semaphore()
        for r in range(nrow):
            for c in range(ncol):
                pl.semaphore_signal(barrier, inc=1, device_id=(r, c), device_id_type=MESH)
    with scope("inputs"):
        for k in (0, 1):
            loads[k].wait()
    valid = valid_ref[0]

    lanes = lax.broadcasted_iota(jnp.int32, (1, 128), 1)
    lane_col = my_col * cols_dev + lanes % cols_dev
    lane_row = my_row * rows_dev + (lanes // cols_dev) * tiles

    def edge(side, t):
        first = 2 * side * width
        if side == 0:
            rows = jnp.concatenate([pair_ref[g * tiles + t] for g in range(group)], axis=0)
            normed_s[t] = norm(rows, 1).astype(BF16)
        proj = jnp.dot(
            normed_s[t], tri_in_ref[:, first : first + 2 * width], preferred_element_type=F32
        )
        keep = jnp.where((lane_row + t < valid) & (lane_col < valid), 1.0, 0.0)
        return jnp.transpose(jax.nn.sigmoid(proj[:, :width]) * proj[:, width:]) * keep

    def left_edges(hh):
        for tt in range(high):
            edge_f[0, pl.ds(hh * width * high + tt, width, stride=high), :] = edge(0, hh * high + tt)
        for d in range(ndev):
            for c in range(chans):
                at = hh * width * high + (c * ndev + d) * high
                left_send[hh, d, c * high : (c + 1) * high] = edge_f[0, at : at + high, :].astype(BF16)

    def right_edges():
        for t in range(tiles):
            edge_f[1, pl.ds(t, width, stride=tiles), :] = edge(1, t)
        for c in range(chans):
            right_send[c] = edge_f[1, pl.ds(c * ndev * tiles, ndev * tiles), :].astype(BF16)

    def share(peer):
        return pl.ds(pl.multiple_of(peer * tiles, tiles), tiles)

    def remote(src, dst, send, recv, where):
        return pltpu.make_async_remote_copy(
            src_ref=src, dst_ref=dst, send_sem=send, recv_sem=recv, device_id=where, device_id_type=MESH
        )

    def left_copy(hh, step):
        peer, where = other(step)
        return remote(left_send.at[hh, peer], left_recv.at[hh, me], send_l.at[hh], recv_l.at[hh], where)

    def right_copy(part, step):
        peer, where = other(step)
        some = pl.ds(part * each, each)
        return remote(
            right_send.at[some, share(peer), :], right_recv.at[part, me],
            send_r.at[part], recv_r.at[part], where,
        )

    for hh in range(halves):
        with scope("edges0"):
            left_edges(hh)
        if hh == 0:
            with scope("barrier"):
                pl.semaphore_wait(barrier, ndev)
        with scope("sendl"):
            loop(ndev, lambda step: left_copy(hh, step).start())
            left_recv[hh, me] = left_send[hh, me]
    with scope("edges1"):
        right_edges()
    with scope("sendr"):
        for part in range(parts):
            loop(ndev, lambda step: right_copy(part, step).start())
            right_recv[part, me] = right_send[part * each : (part + 1) * each, share(me), :]
    with scope("gate"):
        for k in (2, 3, 5, 4, 6):
            loads[k].wait()
        tri_out_s[...] = jnp.transpose(tri_out_ref[...].astype(F32)).astype(BF16)
        for t in range(tiles):
            tri_gate_s[t] = jax.nn.sigmoid(
                lax.dot_general(
                    tri_gate_ref[...], normed_s[t], (((0,), (1,)), ((), ())), preferred_element_type=F32
                )
            )
            rows = jnp.concatenate([pair_ref[g * tiles + t] for g in range(group)], axis=0)
            pair_s[t] = jnp.transpose(rows)
    others = pl.ds(0, ndev - 1)
    with scope("waitl"):
        for hh in range(halves):
            arrived(left_recv.at[hh, others], recv_l.at[hh])

    lane = lax.broadcasted_iota(jnp.int32, (tiles, 128), 1) // cols_dev

    def spread(load, operand):
        for r in range(nrow):
            for half in range(ncol // group):
                blocks = [load(r * ncol + half * group + a) for a in range(group)]
                for b, piece in enumerate(swap_groups(blocks, lane, cols_dev)):
                    operand[
                        pl.ds(r * rows_dev + b * tiles, tiles), pl.ds(half * 128, 128)
                    ] = piece.astype(BF16)

    def prod_copy(part, hh, step):
        peer, where = other(step)
        some = pl.ds(part * each * high, each * high)
        return remote(
            prod_send.at[peer, hh, some], prod_recv.at[hh, part, me],
            send_p.at[part, hh], recv_p.at[part, hh], where,
        )

    with scope("spreadl"):
        for c in range(chans):
            spread(
                lambda d: jnp.concatenate(
                    [left_recv[hh, d, c * high : (c + 1) * high].astype(F32) for hh in range(halves)], axis=0
                ),
                left_s.at[c],
            )
    for part in range(parts):
        with scope("waitr"):
            arrived(right_recv.at[part, others], recv_r.at[part])
        with scope("products"):
            for c in range(part * each, (part + 1) * each):
                spread(lambda d: right_recv[part, d, c - part * each].astype(F32), right_s.at[c])
                products = lax.dot_general(
                    left_s[c], right_s[c], (((1,), (1,)), ((), ())), preferred_element_type=F32
                )
                for r in range(nrow):
                    for half in range(ncol // group):
                        blocks = [
                            products[
                                r * rows_dev + a * tiles : r * rows_dev + (a + 1) * tiles,
                                half * 128 : (half + 1) * 128,
                            ]
                            for a in range(group)
                        ]
                        for b, piece in enumerate(swap_groups(blocks, lane, cols_dev)):
                            for hh in range(halves):
                                prod_send[r * ncol + half * group + b, hh, c * high : (c + 1) * high] = piece[
                                    hh * high : (hh + 1) * high
                                ].astype(BF16)
        with scope("sendp"):
            for hh in range(halves if part == parts - 1 else 1):
                for p in range(part if hh == 0 else 0, part + 1):
                    loop(ndev, lambda step: prod_copy(p, hh, step).start())
                    prod_recv[hh, p, me] = prod_send[me, hh, p * each * high : (p + 1) * each * high]

    def strip(peer):
        return pl.ds(pl.multiple_of(peer * cols_dev, cols_dev), cols_dev)

    def send_rows(t):
        i = t // span
        for g in range(group):
            turn = lax.rem(g + my_z, group)
            owner = turn * span + t % span

            @pl.when(owner != my_col)
            def _():
                remote(
                    mid_send.at[t, strip(turn), :], mid_recv.at[i, strip(my_col), :],
                    send_m, recv_m.at[i], (my_row, owner),
                ).start()

            @pl.when(owner == my_col)
            def _():
                mid_recv[i, strip(my_col), :] = mid_send[t, strip(turn), :]

    def bias_block(hh, z):
        block = bias_recv.at[core, hh, my_row, z]
        for step in range(1, nrow):
            peer = lax.rem(my_row + step, nrow)
            remote(block, block, send_b.at[1, hh], recv_b.at[1, hh], (peer, my_col)).start()

    def bias_z(hh):
        mine = bias_recv.at[core, hh, my_row, my_z]
        for step in range(1, nz):
            peer = lax.rem(my_z + step, nz)
            remote(mine, mine, send_b.at[0, hh], recv_z.at[hh, my_z], (my_row, 2 * peer + core)).start()
        bias_block(hh, my_z)

    def bias_row(hh):
        turn = 1 - 2 * (my_z // (nz // 2))
        for step in range(1, nz):
            z = lax.rem(my_z + turn * step + nz, nz)
            arrived(bias_recv.at[0, hh, 0, 0], recv_z.at[hh, z])
            bias_block(hh, z)

    def bias_hand(hh):
        mine = bias_recv.at[core, hh]
        return remote(mine, mine, send_b.at[2, hh], recv_b.at[2, hh], (my_row, my_col + 1 - 2 * core))

    def bias_core(hh):
        arrived(bias_recv.at[0, hh, pl.ds(0, nrow - 1)], recv_b.at[1, hh])
        bias_hand(hh).start()

    for hh in range(halves):
        with scope("waitp"):
            for part in range(parts):
                arrived(prod_recv.at[hh, part, others], recv_p.at[part, hh])
        with scope("unpack"):
            for part in range(parts):
                for d in range(ndev):
                    for c in range(each):
                        at = ((part * each + c) * ndev + d) * high
                        prod_f[at : at + high, :] = prod_recv[hh, part, d, c * high : (c + 1) * high].astype(F32)
        with scope("middle"):
            for tt in range(high):
                t = hh * high + tt
                prods = norm(prod_f[pl.ds(tt, width, stride=high), :], 0).astype(BF16)
                update = jnp.dot(tri_out_s[...], prods, preferred_element_type=F32)
                middle = pair_s[t] + tri_gate_s[t] * update
                middle_s[t] = middle
                normed_mid = norm(middle, 0)
                own = jnp.dot(bias_w_ref[...], normed_mid.astype(BF16), preferred_element_type=F32)
                for h in range(heads):
                    bias_f[pl.ds(h * high + tt, 1), :] = own[h : h + 1]
                mid_send[t] = jnp.transpose(normed_mid).astype(BF16)
        with scope("bias_z"):
            bias_recv[core, hh, my_row, my_z] = bias_f[...].astype(BF16)
            bias_z(hh)
        with scope("send_rows"):
            early = range(3 * high // 4) if hh == 0 and halves > 1 else range(high)
            if hh > 0:
                for tt in range(3 * high // 4 if hh == 1 else high, high):
                    send_rows((hh - 1) * high + tt)
            for tt in early:
                send_rows(hh * high + tt)

    def take(i):
        arrived(mid_recv.at[i, pl.ds(0, (ncol - 1) * cols_dev), :], recv_m.at[i])

    tokens = lax.broadcasted_iota(jnp.int32, (1, total), 1)
    mask = jnp.where(tokens < valid, 0.0, -1000000000.0)
    narrow = lax.broadcasted_iota(jnp.int32, (high, 128), 1) // cols_dev

    def assemble(hh):
        arrived(bias_recv.at[0, hh], recv_b.at[2, hh])
        for h in range(heads):
            for r in range(nrow):
                for half in range(ncol // group):
                    blocks = []
                    for a in range(group):
                        c = half * group + a
                        blocks.append(
                            bias_recv[c % 2, hh, r, c // 2, h * high : (h + 1) * high, :].astype(F32)
                        )
                    for b, piece in enumerate(swap_groups(blocks, narrow, cols_dev)):
                        bias_full[
                            hh, h, pl.ds((r * group + b) * high, high), pl.ds(half * 128, 128)
                        ] = piece + mask[:, half * 128 : (half + 1) * 128]

    def project(i):
        with scope("take"):
            take(i)
        with scope("project"):
            proj = jnp.dot(mid_recv[i], att_in_ref[...], preferred_element_type=F32)
            kv_s[i] = proj[:, width : 3 * width].astype(BF16)
            query = proj[:, :width] * head_size ** (-0.5)
            gate = jax.nn.sigmoid(proj[:, 3 * width :])
            for hh in range(halves):
                pick = lambda x: jnp.concatenate(
                    [x[at : at + high] for at in range(hh * high, total, tiles)], axis=0
                )
                query_s[i, hh] = pick(query).astype(BF16)
                gate_s[i, hh] = pick(gate)

    with scope("bias_row"):
        bias_row(0)
    with scope("keep_middle"):
        for t in range(tiles):
            middle = jnp.transpose(middle_s[t])
            for g in range(group):
                out_ref[g * tiles + t] = middle[g * cols_dev : (g + 1) * cols_dev]
    with scope("bias_core"):
        bias_core(0)

    block = min(128, total // halves)
    own_cols = cols_dev // halves
    head = lax.broadcasted_iota(jnp.int32, (block, width), 1) // head_size

    def share_cols(peer):
        return pl.ds(pl.multiple_of(peer * own_cols, own_cols), own_cols)

    def home_copy(hh, i, step):
        peer = lax.rem(my_col + step, ncol)
        return remote(
            gated_s.at[hh, i, share_cols(peer), :], gated_recv.at[hh, i, share_cols(my_col), :],
            send_g, recv_g.at[hh, i], (my_row, peer),
        )

    def attend(hh, i):
        keys = kv_s[i, :, :width]
        values = jnp.concatenate([kv_s[i, :, width:], jnp.ones((total, width), BF16)], axis=1)
        for first in range(0, total // halves, block):
            query = query_s[i, hh, first : first + block, :]
            top = jnp.zeros((block, width), F32)
            bottom = jnp.ones((block, width), F32)
            for h in range(heads):
                scores = lax.dot_general(
                    jnp.where(head == h, query, jnp.zeros_like(query)), keys,
                    (((1,), (1,)), ((), ())), preferred_element_type=F32,
                )
                scores = scores + bias_full[hh, h, first : first + block, :]
                expo = jnp.exp(scores - jnp.max(scores, axis=1, keepdims=True)).astype(BF16)
                both = jnp.dot(expo, values, preferred_element_type=F32)
                top = jnp.where(head == h, both[:, :width], top)
                bottom = jnp.where(head == h, both[:, width:], bottom)
            gated_s[hh, i, first : first + block, :] = (
                gate_s[i, hh, first : first + block, :] * top / bottom
            ).astype(BF16)
        for step in range(1, ncol):
            home_copy(hh, i, step).start()
        gated_recv[hh, i, share_cols(my_col), :] = gated_s[hh, i, share_cols(my_col), :]

    def run(first, last, act):
        def body(i, carry):
            act(i)
            return carry

        lax.fori_loop(first, last, body, 0)

    def first_pass(i):
        project(i)
        attend(0, i)

    ready = per // halves
    project(0)
    with scope("bias_row"):
        for hh in range(1, halves):
            bias_row(hh)
    with scope("assemble"):
        assemble(0)
    with scope("attend"):
        attend(0, 0)
        run(1, ready, first_pass)
    with scope("bias_core"):
        for hh in range(1, halves):
            bias_core(hh)
    with scope("attend"):
        run(ready, per, first_pass)
    for hh in range(1, halves):
        with scope("assemble"):
            assemble(hh)
        with scope("attend"):
            run(0, per, lambda i: attend(hh, i))

    def finish(hh, i):
        with scope("waitg"):
            arrived(gated_recv.at[hh, i, pl.ds(0, (ncol - 1) * own_cols), :], recv_g.at[hh, i])
        added = jnp.dot(gated_recv[hh, i], att_out_ref[...], preferred_element_type=F32)
        for q in range(ncol):
            row = (q // span) * tiles + i * span + q % span
            for m in range(own_cols // high):
                at = q * own_cols + m * high
                out_ref[row, m * tiles + hh * high : m * tiles + (hh + 1) * high] += added[at : at + high]

    with scope("finish"):
        for hh in range(halves):
            run(0, per, lambda i: finish(hh, i))
    with scope("drain"):
        for hh in range(halves):
            arrived(left_recv.at[hh, others], send_l.at[hh])
        for part in range(parts):
            arrived(right_recv.at[part, others], send_r.at[part])
            for hh in range(halves):
                arrived(prod_recv.at[hh, part, others], send_p.at[part, hh])
        for i in range(per):
            arrived(mid_recv.at[i, pl.ds(0, (ncol - 1) * cols_dev), :], send_m)
            arrived(mid_recv.at[i, pl.ds(0, (ncol - 1) * cols_dev), :], send_g)
        for hh in range(halves):
            arrived(bias_recv.at[0, hh, 0, pl.ds(0, nz - 1)], send_b.at[0, hh])
            arrived(bias_recv.at[0, hh, pl.ds(0, nrow - 1)], send_b.at[1, hh])
            arrived(bias_recv.at[0, hh], send_b.at[2, hh])


def per_device(pair, valid_length, tri_in, tri_gate, tri_out, att_in, att_bias, att_out):
    rows_dev, cols_dev, width = pair.shape
    heads = att_bias.shape[1]
    nrow, ncol = lax.axis_size("row"), lax.axis_size("col")
    ndev = nrow * ncol
    total = ncol * cols_dev
    tiles = rows_dev // (128 // cols_dev)
    chans = width // ndev
    parts = 2 if chans % 2 == 0 else 1
    each = chans // parts
    per = rows_dev // ncol
    halves = 2 if tiles % 16 == 0 and (tiles // 2) % per == 0 else 1
    high = tiles // halves
    hbm = pl.BlockSpec(memory_space=pltpu.HBM)
    vmem = pl.BlockSpec(memory_space=pltpu.VMEM)
    held = lambda dtype, *shape: pltpu.VMEM(shape, dtype)
    sem = lambda *shape: pltpu.SemaphoreType.DMA(shape) if shape else pltpu.SemaphoreType.DMA
    bias_w = att_bias.T
    args = [pltpu.with_memory_space_constraint(a, pltpu.HBM) for a in (pair, tri_in, tri_gate, tri_out, att_in, bias_w, att_out)]
    return pl.pallas_call(
        functools.partial(kernel, (nrow, ncol, rows_dev, cols_dev, width, heads, parts, halves)),
        out_shape=jax.ShapeDtypeStruct((rows_dev, cols_dev, width), F32),
        in_specs=[pl.BlockSpec(memory_space=pltpu.SMEM)] + [hbm] * 7,
        out_specs=vmem,
        scratch_shapes=[
            *[held(a.dtype, *a.shape) for a in args],
            held(BF16, tiles, 128, width),
            held(F32, 2, width * tiles, 128),
            held(BF16, halves, ndev, chans * high, 128),
            held(BF16, chans, ndev * tiles, 128),
            held(BF16, halves, ndev, chans * high, 128),
            held(BF16, parts, ndev, each, tiles, 128),
            held(BF16, chans, total, total),
            held(BF16, chans, total, total),
            held(BF16, ndev, halves, chans * high, 128),
            held(BF16, halves, parts, ndev, each * high, 128),
            held(F32, width * high, 128),
            held(F32, tiles, width, 128),
            held(F32, tiles, width, 128),
            held(F32, tiles, width, 128),
            held(BF16, width, width),
            held(BF16, tiles, 128, width),
            held(BF16, per, total, width),
            held(BF16, per, total, 2 * width),
            held(BF16, per, halves, total // halves, width),
            held(F32, per, halves, total // halves, width),
            held(F32, heads * high, 128),
            held(BF16, 2, halves, nrow, ncol // 2, heads * high, 128),
            held(F32, halves, heads, total // halves, total),
            held(BF16, halves, per, total // halves, width),
            held(BF16, halves, per, total // halves, width),
            sem(7), sem(halves), sem(halves), sem(parts), sem(parts), sem(parts, halves), sem(parts, halves),
            sem(), sem(per), sem(3, halves), sem(halves, ncol // 2), sem(3, halves), sem(), sem(halves, per),
        ],
        compiler_params=pltpu.CompilerParams(
            collective_id=0, has_side_effects=True, vmem_limit_bytes=40 * 1024 * 1024
        ),
    )(valid_length, *args)


def solution(mesh):
    placed = (P("row", "col", None), P(), P(), P(), P(), P(), P(), P())
    return jax.shard_map(
        per_device, mesh=mesh, in_specs=placed, out_specs=P("row", "col", None), check_vma=False
    )
```

```python
import functools

import jax
import jax.numpy as jnp
from jax import lax
from jax.experimental import pallas as pl
from jax.experimental.pallas import tpu as pltpu
from jax.sharding import PartitionSpec as P

MESH = pl.DeviceIdType.MESH
F32 = jnp.float32
BF16 = jnp.bfloat16
scope = jax.named_scope


def norm(values, axis):
    center = values - jnp.mean(values, axis=axis, keepdims=True)
    return center * lax.rsqrt(jnp.mean(center * center, axis=axis, keepdims=True) + 1e-05)


def swap_groups(blocks, lane, group):
    count = len(blocks)
    width = count * group
    out = []
    for b in range(count):
        total = None
        for a in range(count):
            shift = (group * (a - b)) % width
            moved = blocks[a] if shift == 0 else pltpu.roll(blocks[a], shift, 1)
            total = moved if total is None else jnp.where(lane == a, moved, total)
        out.append(total)
    return out


def arrived(ref, sem):
    pltpu.make_async_copy(ref, ref, sem).wait()


def kernel(
    dims,
    valid_ref, pair_h, tri_in_h, tri_gate_h, tri_out_h, att_in_h, bias_w_h, att_out_h,
    out_ref,
    pair_ref, tri_in_ref, tri_gate_ref, tri_out_ref, att_in_ref, bias_w_ref, att_out_ref,
    tri_in_s, tri_gate_t, tri_out_s, normed_s, pair_s, middle_s, gate_t, edge_f,
    near_send, near_recv, far_send, far_recv, near_left, near_right, far_left, far_right,
    near_psend, near_precv, far_psend, far_precv, prod_f,
    mid_send, mid_recv, kv_s, query_s, gate_s,
    bias_f, bias_recv, bias_full, gated_s, gated_recv,
    sem_in, sem_pair, send_n, recv_n, send_f, recv_f, send_pn, recv_pn, send_pf, recv_pf, send_m, recv_m,
    send_b, recv_z, recv_b, send_g, recv_g,
):
    nrow, ncol, rows_dev, cols_dev, width, heads, far, near, parts, halves = dims
    ndev = nrow * ncol
    total = ncol * cols_dev
    group = 128 // cols_dev
    tiles = rows_dev // group
    each = near // parts if parts else 0
    side_cols = ncol // 2
    team = nrow * side_cols
    per = rows_dev // ncol
    span = tiles // per
    high = tiles // halves
    nz = ncol // 2
    head_size = width // heads
    my_row, my_col = lax.axis_index("row"), lax.axis_index("col")
    me = my_row * ncol + my_col
    core, my_z = lax.rem(my_col, 2), my_col // 2
    my_side, my_rank = my_col // side_cols, my_row * side_cols + lax.rem(my_col, side_cols)

    held = (tri_in_ref, tri_gate_ref, tri_out_ref, att_in_ref, bias_w_ref, att_out_ref)
    given = (tri_in_h, tri_gate_h, tri_out_h, att_in_h, bias_w_h, att_out_h)
    loads = [pltpu.make_async_copy(g, v, sem_in.at[k]) for k, (g, v) in enumerate(zip(given, held))]
    loads[0].start()
    for hh in range(halves):
        for g in range(group):
            some = pl.ds(g * tiles + hh * high, high)
            pltpu.make_async_copy(pair_h.at[some], pair_ref.at[some], sem_pair.at[hh]).start()
    for k in (1, 2, 4, 3, 5):
        loads[k].start()

    def other(step):
        peer = lax.rem(me + step, ndev)
        return peer, (peer // ncol, lax.rem(peer, ncol))

    def loop(count, act):
        def run(step, carry):
            act(step)
            return carry

        lax.fori_loop(1, count, run, 0)

    with scope("signal"):
        barrier = pltpu.get_barrier_semaphore()
        for r in range(nrow):
            for c in range(ncol):
                pl.semaphore_signal(barrier, inc=1, device_id=(r, c), device_id_type=MESH)
    with scope("inputs"):
        loads[0].wait()
        tri_in_s[...] = jnp.transpose(tri_in_ref[...].astype(F32)).astype(BF16)
    valid = valid_ref[0]

    lanes = lax.broadcasted_iota(jnp.int32, (1, 128), 1)
    lane_col = my_col * cols_dev + lanes % cols_dev
    lane_row = my_row * rows_dev + (lanes // cols_dev) * tiles

    def edges(hh):
        arrived(pair_ref.at[pl.ds(0, group * high)], sem_pair.at[hh])
        for tt in range(high):
            t = hh * high + tt
            rows = jnp.concatenate([pair_ref[g * tiles + t] for g in range(group)], axis=0)
            rows = jnp.transpose(rows)
            pair_s[t] = rows
            normed = norm(rows, 0).astype(BF16)
            normed_s[t] = normed
            keep = jnp.where((lane_row + t < valid) & (lane_col < valid), 1.0, 0.0)
            for side in range(2):
                proj = jnp.dot(
                    tri_in_s[2 * side * width : 2 * (side + 1) * width, :], normed, preferred_element_type=F32
                )
                edge_f[side, hh, pl.ds(tt, width, stride=high), :] = (
                    jax.nn.sigmoid(proj[:width]) * proj[width:] * keep
                )

    def near_channel(k, rank):
        return far * ndev + k * team + rank

    def near_pack(part, hh):
        for rank in range(team):
            for side in range(2):
                for k in range(each):
                    at = near_channel(part * each + k, rank) * high
                    near_send[part, hh, rank, side, k * high : (k + 1) * high] = edge_f[
                        side, hh, at : at + high, :
                    ].astype(BF16)

    def far_pack():
        for d in range(ndev):
            for side in range(2):
                for f in range(far):
                    for hh in range(halves):
                        at = (f * ndev + d) * high
                        to = (f * halves + hh) * high
                        far_send[d, side, to : to + high] = edge_f[side, hh, at : at + high, :].astype(BF16)

    def remote(src, dst, send, recv, where):
        return pltpu.make_async_remote_copy(
            src_ref=src, dst_ref=dst, send_sem=send, recv_sem=recv, device_id=where, device_id_type=MESH
        )

    def near_copy(part, hh, step):
        peer = lax.rem(my_rank + step, team)
        return remote(
            near_send.at[part, hh, peer], near_recv.at[part, hh, my_rank],
            send_n.at[part, hh], recv_n.at[part, hh],
            (peer // side_cols, my_side * side_cols + lax.rem(peer, side_cols)),
        )

    def far_copy(step):
        peer, where = other(step)
        return remote(far_send.at[peer], far_recv.at[me], send_f, recv_f, where)

    def near_start(part, hh):
        with scope("near_start"):
            near_pack(part, hh)
            loop(team, lambda step: near_copy(part, hh, step).start())
            near_recv[part, hh, my_rank] = near_send[part, hh, my_rank]

    for hh in range(halves):
        with scope("edges"):
            edges(hh)
        if hh == 0:
            with scope("barrier"):
                pl.semaphore_wait(barrier, ndev)
        if parts:
            near_start(0, hh)
    with scope("far_start"):
        far_pack()
        loop(ndev, lambda step: far_copy(step).start())
        far_recv[me] = far_send[me]
    for part in range(1, parts):
        for hh in range(halves):
            near_start(part, hh)
    with scope("gate"):
        for k in (1, 2, 4, 3, 5):
            loads[k].wait()
        tri_out_s[...] = jnp.transpose(tri_out_ref[...].astype(F32)).astype(BF16)
        tri_gate_t[...] = jnp.transpose(tri_gate_ref[...].astype(F32)).astype(BF16)
        for t in range(tiles):
            gate_t[t] = jax.nn.sigmoid(
                jnp.dot(tri_gate_t[...], normed_s[t], preferred_element_type=F32)
            )
    others = pl.ds(0, ndev - 1)
    team_others = pl.ds(0, team - 1)

    lane = lax.broadcasted_iota(jnp.int32, (tiles, 128), 1) // cols_dev

    def spread(load, columns, operand):
        for r in range(nrow):
            for half in range(columns // group):
                blocks = [load(r * columns + half * group + a) for a in range(group)]
                for b, piece in enumerate(swap_groups(blocks, lane, cols_dev)):
                    operand[
                        pl.ds(r * rows_dev + b * tiles, tiles), pl.ds(half * 128, 128)
                    ] = piece.astype(BF16)

    def multiply(left, right, put):
        products = lax.dot_general(left, right, (((1,), (1,)), ((), ())), preferred_element_type=F32)
        for r in range(nrow):
            for half in range(ncol // group):
                blocks = [
                    products[
                        r * rows_dev + a * tiles : r * rows_dev + (a + 1) * tiles,
                        half * 128 : (half + 1) * 128,
                    ]
                    for a in range(group)
                ]
                for b, piece in enumerate(swap_groups(blocks, lane, cols_dev)):
                    for hh in range(halves):
                        put(r * ncol + half * group + b, hh, piece[hh * high : (hh + 1) * high].astype(BF16))

    def near_pcopy(part, hh, step):
        peer, where = other(step)
        return remote(
            near_psend.at[part, hh, peer], near_precv.at[part, hh, me],
            send_pn.at[part, hh], recv_pn.at[part, hh], where,
        )

    def far_pcopy(step):
        peer, where = other(step)
        return remote(far_psend.at[peer], far_precv.at[me], send_pf, recv_pf, where)

    def near_products(part):
        for hh in range(halves):
            with scope("near_wait"):
                arrived(near_recv.at[part, hh, team_others], recv_n.at[part, hh])
        with scope("near_products"):
            for k in range(each):
                for side, operand in ((0, near_left), (1, near_right)):
                    spread(
                        lambda d: jnp.concatenate(
                            [
                                near_recv[part, hh, d, side, k * high : (k + 1) * high].astype(F32)
                                for hh in range(halves)
                            ],
                            axis=0,
                        ),
                        side_cols, operand.at[k],
                    )

                def put(d, hh, piece):
                    near_psend[part, hh, d, k * high : (k + 1) * high] = piece

                multiply(near_left[k], near_right[k], put)
        with scope("near_psend"):
            for hh in range(halves):
                loop(ndev, lambda step: near_pcopy(part, hh, step).start())
                near_precv[part, hh, me] = near_psend[part, hh, me]

    def far_products():
        with scope("far_wait"):
            arrived(far_recv.at[others], recv_f)
        with scope("far_products"):
            for f in range(far):
                for side, operand in ((0, far_left), (1, far_right)):
                    spread(
                        lambda d: far_recv[d, side, f * tiles : (f + 1) * tiles].astype(F32), ncol, operand.at[f]
                    )

                def put(d, hh, piece):
                    at = (f * halves + hh) * high
                    far_psend[d, at : at + high] = piece

                multiply(far_left[f], far_right[f], put)
        with scope("far_psend"):
            loop(ndev, lambda step: far_pcopy(step).start())
            far_precv[me] = far_psend[me]

    for part in range(parts):
        if part == 1:
            far_products()
        near_products(part)
    if parts < 2:
        far_products()

    def strip(peer):
        return pl.ds(pl.multiple_of(peer * cols_dev, cols_dev), cols_dev)

    def send_rows(t):
        i = t // span
        for g in range(group):
            turn = lax.rem(g + my_z, group)
            owner = turn * span + t % span

            @pl.when(owner != my_col)
            def _():
                remote(
                    mid_send.at[t, strip(turn), :], mid_recv.at[i, strip(my_col), :],
                    send_m, recv_m.at[i], (my_row, owner),
                ).start()

            @pl.when(owner == my_col)
            def _():
                mid_recv[i, strip(my_col), :] = mid_send[t, strip(turn), :]

    def bias_block(hh, z):
        block = bias_recv.at[core, hh, my_row, z]
        for step in range(1, nrow):
            peer = lax.rem(my_row + step, nrow)
            remote(block, block, send_b.at[1, hh], recv_b.at[1, hh], (peer, my_col)).start()

    def bias_z(hh):
        mine = bias_recv.at[core, hh, my_row, my_z]
        for step in range(1, nz):
            peer = lax.rem(my_z + step, nz)
            remote(mine, mine, send_b.at[0, hh], recv_z.at[hh, my_z], (my_row, 2 * peer + core)).start()
        bias_block(hh, my_z)

    def bias_row(hh):
        turn = 1 - 2 * (my_z // (nz // 2))
        for step in range(1, nz):
            z = lax.rem(my_z + turn * step + nz, nz)
            arrived(bias_recv.at[0, hh, 0, 0], recv_z.at[hh, z])
            bias_block(hh, z)

    def bias_hand(hh):
        mine = bias_recv.at[core, hh]
        return remote(mine, mine, send_b.at[2, hh], recv_b.at[2, hh], (my_row, my_col + 1 - 2 * core))

    def bias_core(hh):
        arrived(bias_recv.at[0, hh, pl.ds(0, nrow - 1)], recv_b.at[1, hh])
        bias_hand(hh).start()

    for hh in range(halves):
        with scope("waitp"):
            if hh == 0:
                arrived(far_precv.at[others], recv_pf)
            for part in range(parts):
                arrived(near_precv.at[part, hh, others], recv_pn.at[part, hh])
        with scope("unpack"):
            for f in range(far):
                for d in range(ndev):
                    at = (f * ndev + d) * high
                    of = (f * halves + hh) * high
                    prod_f[at : at + high, :] = far_precv[d, of : of + high].astype(F32)
            for part in range(parts):
                for rank in range(team):
                    one = (rank // side_cols) * ncol + rank % side_cols
                    for k in range(each):
                        at = near_channel(part * each + k, rank) * high
                        of = slice(k * high, (k + 1) * high)
                        prod_f[at : at + high, :] = near_precv[part, hh, one, of].astype(F32) + near_precv[
                            part, hh, one + side_cols, of
                        ].astype(F32)
        with scope("middle"):
            for tt in range(high):
                t = hh * high + tt
                prods = norm(prod_f[pl.ds(tt, width, stride=high), :], 0).astype(BF16)
                update = jnp.dot(tri_out_s[...], prods, preferred_element_type=F32)
                middle = pair_s[t] + gate_t[t] * update
                middle_s[t] = middle
                normed_mid = norm(middle, 0)
                own = jnp.dot(bias_w_ref[...], normed_mid.astype(BF16), preferred_element_type=F32)
                for h in range(heads):
                    bias_f[pl.ds(h * high + tt, 1), :] = own[h : h + 1]
                mid_send[t] = jnp.transpose(normed_mid).astype(BF16)
        with scope("bias_z"):
            bias_recv[core, hh, my_row, my_z] = bias_f[...].astype(BF16)
            bias_z(hh)
        with scope("send_rows"):
            early = range(3 * high // 4) if hh == 0 and halves > 1 else range(high)
            if hh > 0:
                for tt in range(3 * high // 4 if hh == 1 else high, high):
                    send_rows((hh - 1) * high + tt)
            for tt in early:
                send_rows(hh * high + tt)

    def take(i):
        arrived(mid_recv.at[i, pl.ds(0, (ncol - 1) * cols_dev), :], recv_m.at[i])

    tokens = lax.broadcasted_iota(jnp.int32, (1, total), 1)
    mask = jnp.where(tokens < valid, 0.0, -1000000000.0)
    narrow = lax.broadcasted_iota(jnp.int32, (high, 128), 1) // cols_dev

    def assemble(hh):
        arrived(bias_recv.at[0, hh], recv_b.at[2, hh])
        for h in range(heads):
            for r in range(nrow):
                for half in range(ncol // group):
                    blocks = []
                    for a in range(group):
                        c = half * group + a
                        blocks.append(
                            bias_recv[c % 2, hh, r, c // 2, h * high : (h + 1) * high, :].astype(F32)
                        )
                    for b, piece in enumerate(swap_groups(blocks, narrow, cols_dev)):
                        bias_full[
                            hh, h, pl.ds((r * group + b) * high, high), pl.ds(half * 128, 128)
                        ] = piece + mask[:, half * 128 : (half + 1) * 128]

    def project(i):
        with scope("take"):
            take(i)
        with scope("project"):
            proj = jnp.dot(mid_recv[i], att_in_ref[...], preferred_element_type=F32)
            kv_s[i] = proj[:, width : 3 * width].astype(BF16)
            query = proj[:, :width] * head_size ** (-0.5)
            gate = jax.nn.sigmoid(proj[:, 3 * width :])
            for hh in range(halves):
                pick = lambda x: jnp.concatenate(
                    [x[at : at + high] for at in range(hh * high, total, tiles)], axis=0
                )
                query_s[i, hh] = pick(query).astype(BF16)
                gate_s[i, hh] = pick(gate)

    with scope("bias_row"):
        bias_row(0)
    with scope("keep_middle"):
        for t in range(tiles):
            middle = jnp.transpose(middle_s[t])
            for g in range(group):
                out_ref[g * tiles + t] = middle[g * cols_dev : (g + 1) * cols_dev]
    with scope("bias_core"):
        bias_core(0)

    block = min(128, total // halves)
    own_cols = cols_dev // halves
    head = lax.broadcasted_iota(jnp.int32, (block, width), 1) // head_size

    def share_cols(peer):
        return pl.ds(pl.multiple_of(peer * own_cols, own_cols), own_cols)

    def home_copy(hh, i, step):
        peer = lax.rem(my_col + step, ncol)
        return remote(
            gated_s.at[hh, i, share_cols(peer), :], gated_recv.at[hh, i, share_cols(my_col), :],
            send_g, recv_g.at[hh, i], (my_row, peer),
        )

    def attend(hh, i):
        keys = kv_s[i, :, :width]
        values = jnp.concatenate([kv_s[i, :, width:], jnp.ones((total, width), BF16)], axis=1)
        for first in range(0, total // halves, block):
            query = query_s[i, hh, first : first + block, :]
            top = jnp.zeros((block, width), F32)
            bottom = jnp.ones((block, width), F32)
            for h in range(heads):
                scores = lax.dot_general(
                    jnp.where(head == h, query, jnp.zeros_like(query)), keys,
                    (((1,), (1,)), ((), ())), preferred_element_type=F32,
                )
                scores = scores + bias_full[hh, h, first : first + block, :]
                expo = jnp.exp(scores - jnp.max(scores, axis=1, keepdims=True)).astype(BF16)
                both = jnp.dot(expo, values, preferred_element_type=F32)
                top = jnp.where(head == h, both[:, :width], top)
                bottom = jnp.where(head == h, both[:, width:], bottom)
            gated_s[hh, i, first : first + block, :] = (
                gate_s[i, hh, first : first + block, :] * top / bottom
            ).astype(BF16)
        for step in range(1, ncol):
            home_copy(hh, i, step).start()
        gated_recv[hh, i, share_cols(my_col), :] = gated_s[hh, i, share_cols(my_col), :]

    def run(first, last, act):
        def body(i, carry):
            act(i)
            return carry

        lax.fori_loop(first, last, body, 0)

    def first_pass(i):
        project(i)
        attend(0, i)

    ready = per // halves
    project(0)
    with scope("bias_row"):
        for hh in range(1, halves):
            bias_row(hh)
    with scope("assemble"):
        assemble(0)
    with scope("attend"):
        attend(0, 0)
        run(1, ready, first_pass)
    with scope("bias_core"):
        for hh in range(1, halves):
            bias_core(hh)
    with scope("attend"):
        run(ready, per, first_pass)
    for hh in range(1, halves):
        with scope("assemble"):
            assemble(hh)
        with scope("attend"):
            run(0, per, lambda i: attend(hh, i))

    def finish(hh, i):
        with scope("waitg"):
            arrived(gated_recv.at[hh, i, pl.ds(0, (ncol - 1) * own_cols), :], recv_g.at[hh, i])
        added = jnp.dot(gated_recv[hh, i], att_out_ref[...], preferred_element_type=F32)
        for q in range(ncol):
            row = (q // span) * tiles + i * span + q % span
            for m in range(own_cols // high):
                at = q * own_cols + m * high
                out_ref[row, m * tiles + hh * high : m * tiles + (hh + 1) * high] += added[at : at + high]

    with scope("finish"):
        for hh in range(halves):
            run(0, per, lambda i: finish(hh, i))
    with scope("drain"):
        arrived(far_recv.at[others], send_f)
        arrived(far_precv.at[others], send_pf)
        for part in range(parts):
            for hh in range(halves):
                arrived(near_recv.at[part, hh, team_others], send_n.at[part, hh])
                arrived(near_precv.at[part, hh, others], send_pn.at[part, hh])
        for i in range(per):
            arrived(mid_recv.at[i, pl.ds(0, (ncol - 1) * cols_dev), :], send_m)
            arrived(mid_recv.at[i, pl.ds(0, (ncol - 1) * cols_dev), :], send_g)
        for hh in range(halves):
            arrived(bias_recv.at[0, hh, 0, pl.ds(0, nz - 1)], send_b.at[0, hh])
            arrived(bias_recv.at[0, hh, pl.ds(0, nrow - 1)], send_b.at[1, hh])
            arrived(bias_recv.at[0, hh], send_b.at[2, hh])


def per_device(pair, valid_length, tri_in, tri_gate, tri_out, att_in, att_bias, att_out):
    rows_dev, cols_dev, width = pair.shape
    heads = att_bias.shape[1]
    nrow, ncol = lax.axis_size("row"), lax.axis_size("col")
    ndev = nrow * ncol
    total = ncol * cols_dev
    tiles = rows_dev // (128 // cols_dev)
    chans = width // ndev
    far = max(1, chans // 4)
    near = 2 * (chans - far)
    parts = 2 if near else 0
    each = near // 2
    team = ndev // 2
    side = ncol // 2 * cols_dev
    per = rows_dev // ncol
    halves = 2 if tiles % 16 == 0 and (tiles // 2) % per == 0 else 1
    high = tiles // halves
    hbm = pl.BlockSpec(memory_space=pltpu.HBM)
    vmem = pl.BlockSpec(memory_space=pltpu.VMEM)
    held = lambda dtype, *shape: pltpu.VMEM(shape, dtype)
    sem = lambda *shape: pltpu.SemaphoreType.DMA(shape) if shape else pltpu.SemaphoreType.DMA
    near_held = lambda *shape: held(BF16, *((parts,) + shape if parts else (1, 8, 128)))
    near_sem = lambda: sem(max(parts, 1), halves)
    bias_w = att_bias.T
    args = [pltpu.with_memory_space_constraint(a, pltpu.HBM) for a in (pair, tri_in, tri_gate, tri_out, att_in, bias_w, att_out)]
    return pl.pallas_call(
        functools.partial(kernel, (nrow, ncol, rows_dev, cols_dev, width, heads, far, near, parts, halves)),
        out_shape=jax.ShapeDtypeStruct((rows_dev, cols_dev, width), F32),
        in_specs=[pl.BlockSpec(memory_space=pltpu.SMEM)] + [hbm] * 7,
        out_specs=vmem,
        scratch_shapes=[
            *[held(a.dtype, *a.shape) for a in args],
            held(BF16, 4 * width, width), held(BF16, width, width), held(BF16, width, width),
            held(BF16, tiles, width, 128),
            held(F32, tiles, width, 128), held(F32, tiles, width, 128), held(F32, tiles, width, 128),
            held(F32, 2, halves, width * high, 128),
            near_held(halves, team, 2, each * high, 128), near_held(halves, team, 2, each * high, 128),
            held(BF16, ndev, 2, far * tiles, 128), held(BF16, ndev, 2, far * tiles, 128),
            held(BF16, max(each, 1), total, side), held(BF16, max(each, 1), total, side),
            held(BF16, far, total, total), held(BF16, far, total, total),
            near_held(halves, ndev, each * high, 128), near_held(halves, ndev, each * high, 128),
            held(BF16, ndev, far * tiles, 128), held(BF16, ndev, far * tiles, 128),
            held(F32, width * high, 128),
            held(BF16, tiles, 128, width),
            held(BF16, per, total, width),
            held(BF16, per, total, 2 * width),
            held(BF16, per, halves, total // halves, width),
            held(F32, per, halves, total // halves, width),
            held(F32, heads * high, 128),
            held(BF16, 2, halves, nrow, ncol // 2, heads * high, 128),
            held(F32, halves, heads, total // halves, total),
            held(BF16, halves, per, total // halves, width),
            held(BF16, halves, per, total // halves, width),
            sem(6), sem(halves), near_sem(), near_sem(), sem(), sem(), near_sem(), near_sem(), sem(), sem(),
            sem(), sem(per), sem(3, halves), sem(halves, ncol // 2), sem(3, halves), sem(), sem(halves, per),
        ],
        compiler_params=pltpu.CompilerParams(
            collective_id=0, has_side_effects=True, vmem_limit_bytes=40 * 1024 * 1024
        ),
    )(valid_length, *args)


def solution(mesh):
    placed = (P("row", "col", None), P(), P(), P(), P(), P(), P(), P())
    return jax.shard_map(
        per_device, mesh=mesh, in_specs=placed, out_specs=P("row", "col", None), check_vma=False
    )
```

```python
import functools

import jax
import jax.numpy as jnp
from jax import lax
from jax.experimental import pallas as pl
from jax.experimental.pallas import tpu as pltpu
from jax.sharding import PartitionSpec as P

MESH = pl.DeviceIdType.MESH
F32 = jnp.float32
BF16 = jnp.bfloat16
scope = jax.named_scope
PAIR = 2


def norm(values, axis):
    center = values - jnp.mean(values, axis=axis, keepdims=True)
    return center * lax.rsqrt(jnp.mean(center * center, axis=axis, keepdims=True) + 1e-05)


def swap_groups(blocks, lane, group):
    count = len(blocks)
    width = count * group
    out = []
    for b in range(count):
        total = None
        for a in range(count):
            shift = (group * (a - b)) % width
            moved = blocks[a] if shift == 0 else pltpu.roll(blocks[a], shift, 1)
            total = moved if total is None else jnp.where(lane == a, moved, total)
        out.append(total)
    return out


def arrived(ref, sem):
    pltpu.make_async_copy(ref, ref, sem).wait()


def kernel(
    dims,
    valid_ref, pair_h, tri_in_h, tri_gate_h, tri_out_h, att_in_h, bias_w_h, att_out_h,
    out_ref,
    pair_ref, tri_in_ref, tri_gate_ref, tri_out_ref, att_in_ref, bias_w_ref, att_out_ref,
    tri_in_s, tri_gate_t, tri_out_s, normed_s, pair_s, middle_s, gate_t, edge_f,
    near_send, near_recv, far_send, far_recv, near_left, near_right, far_left, far_right,
    near_psend, near_precv, far_psend, far_precv, prod_f,
    mid_send, mid_recv, kv_s, query_s, gate_s,
    bias_f, bias_recv, bias_full, gated_s, gated_recv,
    sem_in, sem_pair, sent, recv_n, recv_f, recv_pn, recv_pf, recv_m, recv_z, recv_b, recv_g,
):
    nrow, ncol, rows_dev, cols_dev, width, heads, far, near, parts, halves = dims
    ndev = nrow * ncol
    total = ncol * cols_dev
    group = 128 // cols_dev
    tiles = rows_dev // group
    each = near // parts if parts else 0
    side_cols = ncol // 2
    team = nrow * side_cols
    per = rows_dev // ncol
    span = tiles // per
    high = tiles // halves
    nz = ncol // 2
    head_size = width // heads
    my_row, my_col = lax.axis_index("row"), lax.axis_index("col")
    me = my_row * ncol + my_col
    core, my_z = lax.rem(my_col, 2), my_col // 2
    my_side, my_rank = my_col // side_cols, my_row * side_cols + lax.rem(my_col, side_cols)

    held = (tri_in_ref, tri_gate_ref, tri_out_ref, att_in_ref, bias_w_ref, att_out_ref)
    given = (tri_in_h, tri_gate_h, tri_out_h, att_in_h, bias_w_h, att_out_h)
    loads = [pltpu.make_async_copy(g, v, sem_in.at[k]) for k, (g, v) in enumerate(zip(given, held))]
    loads[0].start()
    for hh in range(halves):
        for g in range(group):
            some = pl.ds(g * tiles + hh * high, high)
            pltpu.make_async_copy(pair_h.at[some], pair_ref.at[some], sem_pair.at[hh]).start()
    for k in (1, 2, 4, 3, 5):
        loads[k].start()

    def other(step):
        peer = lax.rem(me + step, ndev)
        return peer, (peer // ncol, lax.rem(peer, ncol))

    def loop(count, act):
        def run(step, carry):
            act(step)
            return carry

        lax.fori_loop(1, count, run, 0)

    with scope("signal"):
        barrier = pltpu.get_barrier_semaphore()
        for r in range(nrow):
            for c in range(ncol):
                pl.semaphore_signal(barrier, inc=1, device_id=(r, c), device_id_type=MESH)
    with scope("inputs"):
        loads[0].wait()
        tri_in_s[...] = jnp.transpose(tri_in_ref[...].astype(F32)).astype(BF16)
    valid = valid_ref[0]

    lanes = lax.broadcasted_iota(jnp.int32, (1, 128), 1)
    lane_col = my_col * cols_dev + lanes % cols_dev
    lane_row = my_row * rows_dev + (lanes // cols_dev) * tiles

    def edges(hh):
        arrived(pair_ref.at[pl.ds(0, group * high)], sem_pair.at[hh])
        for tt in range(high):
            t = hh * high + tt
            rows = jnp.concatenate([pair_ref[g * tiles + t] for g in range(group)], axis=0)
            rows = jnp.transpose(rows)
            pair_s[t] = rows
            normed = norm(rows, 0).astype(BF16)
            normed_s[t] = normed
            keep = jnp.where((lane_row + t < valid) & (lane_col < valid), 1.0, 0.0)
            for side in range(2):
                proj = jnp.dot(
                    tri_in_s[2 * side * width : 2 * (side + 1) * width, :], normed, preferred_element_type=F32
                )
                edge_f[side, hh, pl.ds(tt, width, stride=high), :] = (
                    jax.nn.sigmoid(proj[:width]) * proj[width:] * keep
                )

    def near_channel(k, rank):
        return far * ndev + k * team + rank

    def near_pack(part, hh):
        for rank in range(team):
            for side in range(2):
                for k in range(each):
                    at = near_channel(part * each + k, rank) * high
                    near_send[part, rank, hh, side, k * high : (k + 1) * high] = edge_f[
                        side, hh, at : at + high, :
                    ].astype(BF16)

    def far_pack():
        for d in range(ndev):
            for side in range(2):
                for f in range(far):
                    for hh in range(halves):
                        at = (f * ndev + d) * high
                        to = (f * halves + hh) * high
                        far_send[d, side, to : to + high] = edge_f[side, hh, at : at + high, :].astype(BF16)

    def remote(src, dst, recv, where):
        return pltpu.make_async_remote_copy(
            src_ref=src, dst_ref=dst, send_sem=sent, recv_sem=recv, device_id=where, device_id_type=MESH
        )

    def near_copy(part, hh, step):
        peer = lax.rem(my_rank + step, team)
        some = pl.ds(0, halves) if hh is None else pl.ds(hh, 1)
        return remote(
            near_send.at[part, peer, some], near_recv.at[part, my_rank, some],
            recv_n.at[part],
            (peer // side_cols, my_side * side_cols + lax.rem(peer, side_cols)),
        )

    def far_copy(step):
        peer, where = other(step)
        return remote(far_send.at[peer], far_recv.at[me], recv_f, where)

    def near_start(part, hh):
        with scope("near_start"):
            loop(team, lambda step: near_copy(part, hh, step).start())

    for hh in range(halves):
        with scope("edges"):
            edges(hh)
        if hh == 0:
            with scope("barrier"):
                pl.semaphore_wait(barrier, ndev)
        if parts:
            near_pack(0, hh)
            near_start(0, hh)
    if far:
        with scope("far_start"):
            far_pack()
            loop(ndev, lambda step: far_copy(step).start())
            far_recv[me] = far_send[me]
    for part in range(parts):
        for hh in range(halves):
            if part:
                near_pack(part, hh)
        near_recv[part, my_rank] = near_send[part, my_rank]
    for part in range(1, parts):
        near_start(part, None)
    with scope("gate"):
        for k in (1, 2, 4, 3, 5):
            loads[k].wait()
        tri_out_s[...] = jnp.transpose(tri_out_ref[...].astype(F32)).astype(BF16)
        tri_gate_t[...] = jnp.transpose(tri_gate_ref[...].astype(F32)).astype(BF16)
        for t in range(tiles):
            gate_t[t] = jax.nn.sigmoid(
                jnp.dot(tri_gate_t[...], normed_s[t], preferred_element_type=F32)
            )
    others = pl.ds(0, ndev - 1)
    chunks = [(i, 1) for i in range(per)]
    ready = per // halves
    waiting = []
    last = halves - 1
    team_others = pl.ds(0, team - 1)

    lane = lax.broadcasted_iota(jnp.int32, (tiles, 128), 1) // cols_dev

    def spread(load, columns, operand):
        for r in range(nrow):
            for half in range(columns // group):
                blocks = [load(r * columns + half * group + a) for a in range(group)]
                for b, piece in enumerate(swap_groups(blocks, lane, cols_dev)):
                    operand[
                        pl.ds(r * rows_dev + b * tiles, tiles), pl.ds(half * 128, 128)
                    ] = piece.astype(BF16)

    def multiply(left, right, put):
        products = lax.dot_general(left, right, (((1,), (1,)), ((), ())), preferred_element_type=F32)
        for r in range(nrow):
            for half in range(ncol // group):
                blocks = [
                    products[
                        r * rows_dev + a * tiles : r * rows_dev + (a + 1) * tiles,
                        half * 128 : (half + 1) * 128,
                    ]
                    for a in range(group)
                ]
                for b, piece in enumerate(swap_groups(blocks, lane, cols_dev)):
                    for hh in range(halves):
                        put(r * ncol + half * group + b, hh, piece[hh * high : (hh + 1) * high].astype(BF16))

    def near_pcopy(part, hh, step):
        peer, where = other(step)
        some = pl.ds(0, halves) if hh is None else pl.ds(hh, 1)
        return remote(
            near_psend.at[part, peer, some], near_precv.at[part, me, some],
            recv_pn.at[part + (hh or 0)], where,
        )

    def far_pcopy(step):
        peer, where = other(step)
        return remote(far_psend.at[peer], far_precv.at[me], recv_pf, where)

    def near_products(part):
        with scope("near_wait"):
            arrived(near_recv.at[part, team_others], recv_n.at[part])
        with scope("near_products"):
            for k in range(each):
                for side, operand in ((0, near_left), (1, near_right)):
                    spread(
                        lambda d: jnp.concatenate(
                            [
                                near_recv[part, d, hh, side, k * high : (k + 1) * high].astype(F32)
                                for hh in range(halves)
                            ],
                            axis=0,
                        ),
                        side_cols, operand.at[k],
                    )

                def put(d, hh, piece):
                    near_psend[part, d, hh, k * high : (k + 1) * high] = piece

                multiply(near_left[k], near_right[k], put)
        with scope("near_psend"):
            for hh in range(halves) if part == parts - 1 else (None,):
                loop(ndev, lambda step: near_pcopy(part, hh, step).start())
            near_precv[part, me] = near_psend[part, me]

    def far_products():
        with scope("far_wait"):
            arrived(far_recv.at[others], recv_f)
        with scope("far_products"):
            for f in range(far):
                for side, operand in ((0, far_left), (1, far_right)):
                    spread(
                        lambda d: far_recv[d, side, f * tiles : (f + 1) * tiles].astype(F32), ncol, operand.at[f]
                    )

                def put(d, hh, piece):
                    at = (f * halves + hh) * high
                    far_psend[d, at : at + high] = piece

                multiply(far_left[f], far_right[f], put)
        with scope("far_psend"):
            loop(ndev, lambda step: far_pcopy(step).start())
            far_precv[me] = far_psend[me]

    for part in range(parts):
        if part == 1 and far:
            far_products()
        near_products(part)
    if parts < 2:
        far_products()

    def strip(peer):
        return pl.ds(pl.multiple_of(peer * cols_dev, cols_dev), cols_dev)

    def send_rows(chunk, steps):
        first, count = chunks[chunk]
        some = pl.ds(first, count)
        for step in steps:
            peer = lax.rem(my_col + step, ncol)
            remote(
                mid_send.at[peer, some], mid_recv.at[some, strip(my_col), :],
                recv_m.at[first // PAIR], (my_row, peer),
            ).start()

    def keep_rows(chunk):
        first, count = chunks[chunk]
        for i in range(first, first + count):
            mid_recv[i, strip(my_col), :] = mid_send[my_col, i]

    def bias_block(hh, z):
        block = bias_recv.at[core, hh, my_row, z]
        for step in range(1, nrow):
            peer = lax.rem(my_row + step, nrow)
            remote(block, block, recv_b.at[0, hh], (peer, my_col)).start()

    def bias_z(hh):
        mine = bias_recv.at[core, hh, my_row, my_z]
        for step in range(1, nz):
            peer = lax.rem(my_z + step, nz)
            remote(mine, mine, recv_z.at[hh if hh < last else last + my_z], (my_row, 2 * peer + core)).start()
        if hh == last:
            bias_block(hh, my_z)

    def bias_row(hh):
        if hh < last:
            arrived(bias_recv.at[0, hh, 0, pl.ds(0, nz - 1)], recv_z.at[hh])
            bias_block(hh, slice(None))
            return
        turn = 1 - 2 * (my_z // (nz // 2))
        for step in range(1, nz):
            z = lax.rem(my_z + turn * step + nz, nz)
            arrived(bias_recv.at[0, hh, 0, 0], recv_z.at[last + z])
            bias_block(hh, z)

    def bias_hand(hh):
        mine = bias_recv.at[core, hh]
        return remote(mine, mine, recv_b.at[1, hh], (my_row, my_col + 1 - 2 * core))

    def bias_core(hh):
        arrived(bias_recv.at[0, hh, pl.ds(0, nrow - 1)], recv_b.at[0, hh])
        bias_hand(hh).start()

    for hh in range(halves):
        with scope("waitp"):
            if hh == 0:
                if far:
                    arrived(far_precv.at[others], recv_pf)
                for part in range(parts - 1):
                    arrived(near_precv.at[part, others], recv_pn.at[part])
            if parts:
                arrived(near_precv.at[parts - 1, others, hh], recv_pn.at[parts - 1 + hh])
        with scope("unpack"):
            for f in range(far):
                for d in range(ndev):
                    at = (f * ndev + d) * high
                    of = (f * halves + hh) * high
                    prod_f[at : at + high, :] = far_precv[d, of : of + high].astype(F32)
            for part in range(parts):
                for rank in range(team):
                    one = (rank // side_cols) * ncol + rank % side_cols
                    for k in range(each):
                        at = near_channel(part * each + k, rank) * high
                        of = slice(k * high, (k + 1) * high)
                        prod_f[at : at + high, :] = near_precv[part, one, hh, of].astype(F32) + near_precv[
                            part, one + side_cols, hh, of
                        ].astype(F32)
        with scope("middle"):
            for tt in range(high):
                t = hh * high + tt
                prods = norm(prod_f[pl.ds(tt, width, stride=high), :], 0).astype(BF16)
                update = jnp.dot(tri_out_s[...], prods, preferred_element_type=F32)
                middle = pair_s[t] + gate_t[t] * update
                middle_s[t] = middle
                normed_mid = norm(middle, 0)
                own = jnp.dot(bias_w_ref[...], normed_mid.astype(BF16), preferred_element_type=F32)
                for h in range(heads):
                    bias_f[pl.ds(h * high + tt, 1), :] = own[h : h + 1]
                normed_mid = jnp.transpose(normed_mid).astype(BF16)
                for g in range(group):
                    mid_send[g * span + t % span, t // span] = normed_mid[g * cols_dev : (g + 1) * cols_dev]
        with scope("bias_z"):
            bias_recv[core, hh, my_row, my_z] = bias_f[...].astype(BF16)
            bias_z(hh)
        with scope("send_rows"):
            fresh = [chunk for chunk, (first, _) in enumerate(chunks) if first // ready == hh]
            held = max(1, len(fresh) // 4) if hh < halves - 1 else 0
            for chunk in waiting + fresh[: len(fresh) - held]:
                send_rows(chunk, range(1, ncol))
                keep_rows(chunk)
            waiting = fresh[len(fresh) - held :]

    def take(i):
        if i % PAIR == 0:
            arrived(mid_recv.at[pl.ds(i, PAIR), pl.ds(0, (ncol - 1) * cols_dev), :], recv_m.at[i // PAIR])

    tokens = lax.broadcasted_iota(jnp.int32, (1, total), 1)
    mask = jnp.where(tokens < valid, 0.0, -1000000000.0)
    narrow = lax.broadcasted_iota(jnp.int32, (high, 128), 1) // cols_dev

    def assemble(hh):
        arrived(bias_recv.at[0, hh], recv_b.at[1, hh])
        for h in range(heads):
            for r in range(nrow):
                for half in range(ncol // group):
                    blocks = []
                    for a in range(group):
                        c = half * group + a
                        blocks.append(
                            bias_recv[c % 2, hh, r, c // 2, h * high : (h + 1) * high, :].astype(F32)
                        )
                    for b, piece in enumerate(swap_groups(blocks, narrow, cols_dev)):
                        bias_full[
                            hh, h, pl.ds((r * group + b) * high, high), pl.ds(half * 128, 128)
                        ] = piece + mask[:, half * 128 : (half + 1) * 128]

    def project(i):
        with scope("take"):
            take(i)
        with scope("project"):
            proj = jnp.dot(mid_recv[i], att_in_ref[...], preferred_element_type=F32)
            kv_s[i] = proj[:, width : 3 * width].astype(BF16)
            query = proj[:, :width] * head_size ** (-0.5)
            gate = jax.nn.sigmoid(proj[:, 3 * width :])
            for hh in range(halves):
                pick = lambda x: jnp.concatenate(
                    [x[at : at + high] for at in range(hh * high, total, tiles)], axis=0
                )
                query_s[i, hh] = pick(query).astype(BF16)
                gate_s[i, hh] = pick(gate)

    with scope("bias_row"):
        bias_row(0)
    with scope("keep_middle"):
        for t in range(tiles):
            middle = jnp.transpose(middle_s[t])
            for g in range(group):
                out_ref[g * tiles + t] = middle[g * cols_dev : (g + 1) * cols_dev]
    with scope("bias_core"):
        bias_core(0)

    block = min(128, total // halves)
    own_cols = cols_dev // halves
    head = lax.broadcasted_iota(jnp.int32, (block, width), 1) // head_size

    def share_cols(peer):
        return pl.ds(pl.multiple_of(peer * own_cols, own_cols), own_cols)

    def home_copy(hh, i, step):
        peer = lax.rem(my_col + step, ncol)
        return remote(
            gated_s.at[hh, i, share_cols(peer), :], gated_recv.at[hh, i, share_cols(my_col), :],
            recv_g.at[hh if hh < last else last + i], (my_row, peer),
        )

    def attend(hh, i):
        keys = kv_s[i, :, :width]
        values = jnp.concatenate([kv_s[i, :, width:], jnp.ones((total, width), BF16)], axis=1)
        for first in range(0, total // halves, block):
            query = query_s[i, hh, first : first + block, :]
            top = jnp.zeros((block, width), F32)
            bottom = jnp.ones((block, width), F32)
            for h in range(heads):
                scores = lax.dot_general(
                    jnp.where(head == h, query, jnp.zeros_like(query)), keys,
                    (((1,), (1,)), ((), ())), preferred_element_type=F32,
                )
                scores = scores + bias_full[hh, h, first : first + block, :]
                expo = jnp.exp(scores - jnp.max(scores, axis=1, keepdims=True)).astype(BF16)
                both = jnp.dot(expo, values, preferred_element_type=F32)
                top = jnp.where(head == h, both[:, :width], top)
                bottom = jnp.where(head == h, both[:, width:], bottom)
            gated_s[hh, i, first : first + block, :] = (
                gate_s[i, hh, first : first + block, :] * top / bottom
            ).astype(BF16)
        for step in range(1, ncol):
            home_copy(hh, i, step).start()
        gated_recv[hh, i, share_cols(my_col), :] = gated_s[hh, i, share_cols(my_col), :]

    def run(first, last, act):
        def body(i, carry):
            act(i)
            return carry

        lax.fori_loop(first, last, body, 0)

    def first_pass(i):
        project(i)
        attend(0, i)

    project(0)
    with scope("bias_row"):
        for hh in range(1, halves):
            bias_row(hh)
    with scope("assemble"):
        assemble(0)
    with scope("attend"):
        attend(0, 0)
        for i in range(1, ready):
            first_pass(i)
    with scope("bias_core"):
        for hh in range(1, halves):
            bias_core(hh)
    with scope("attend"):
        for i in range(ready, per):
            first_pass(i)
    for hh in range(1, halves):
        with scope("assemble"):
            assemble(hh)
        with scope("attend"):
            run(0, per, lambda i: attend(hh, i))

    def finish(hh, i):
        if hh == last:
            with scope("waitg"):
                arrived(gated_recv.at[hh, i, pl.ds(0, (ncol - 1) * own_cols), :], recv_g.at[last + i])
        added = jnp.dot(gated_recv[hh, i], att_out_ref[...], preferred_element_type=F32)
        for q in range(ncol):
            row = (q // span) * tiles + i * span + q % span
            for m in range(own_cols // high):
                at = q * own_cols + m * high
                out_ref[row, m * tiles + hh * high : m * tiles + (hh + 1) * high] += added[at : at + high]

    with scope("finish"):
        for hh in range(halves):
            if hh < last:
                arrived(gated_recv.at[hh, :, pl.ds(0, (ncol - 1) * own_cols), :], recv_g.at[hh])
            run(0, per, lambda i: finish(hh, i))
    with scope("drain"):
        arrived(far_recv.at[others], sent)
        arrived(far_precv.at[others], sent)
        for part in range(parts):
            arrived(near_recv.at[part, team_others], sent)
            for hh in range(halves):
                arrived(near_precv.at[part, others, hh], sent)
        arrived(mid_recv.at[:, pl.ds(0, (ncol - 1) * cols_dev), :], sent)
        for hh in range(halves):
            arrived(gated_recv.at[hh, :, pl.ds(0, (ncol - 1) * own_cols), :], sent)
            arrived(bias_recv.at[0, hh, 0, pl.ds(0, nz - 1)], sent)
            arrived(bias_recv.at[0, hh, pl.ds(0, nrow - 1)], sent)
            arrived(bias_recv.at[0, hh], sent)


def per_device(pair, valid_length, tri_in, tri_gate, tri_out, att_in, att_bias, att_out):
    rows_dev, cols_dev, width = pair.shape
    heads = att_bias.shape[1]
    nrow, ncol = lax.axis_size("row"), lax.axis_size("col")
    ndev = nrow * ncol
    total = ncol * cols_dev
    tiles = rows_dev // (128 // cols_dev)
    chans = width // ndev
    far = max(1, chans // 4)
    near = 2 * (chans - far)
    parts = 2 if near else 0
    each = near // 2
    team = ndev // 2
    side = ncol // 2 * cols_dev
    per = rows_dev // ncol
    halves = 2 if tiles % 16 == 0 and (tiles // 2) % per == 0 else 1
    high = tiles // halves
    hbm = pl.BlockSpec(memory_space=pltpu.HBM)
    held = lambda dtype, *shape: pltpu.VMEM(shape, dtype)
    sem = lambda *shape: pltpu.SemaphoreType.DMA(shape) if shape else pltpu.SemaphoreType.DMA
    near_held = lambda *shape: held(BF16, *((parts,) + shape if parts else (1, 8, 128)))
    bias_w = att_bias.T
    args = [pltpu.with_memory_space_constraint(a, pltpu.HBM) for a in (pair, tri_in, tri_gate, tri_out, att_in, bias_w, att_out)]
    return pl.pallas_call(
        functools.partial(kernel, (nrow, ncol, rows_dev, cols_dev, width, heads, far, near, parts, halves)),
        out_shape=jax.ShapeDtypeStruct((rows_dev, cols_dev, width), F32),
        in_specs=[pl.BlockSpec(memory_space=pltpu.SMEM)] + [hbm] * 7,
        out_specs=pl.BlockSpec(memory_space=pltpu.VMEM),
        scratch_shapes=[
            *[held(a.dtype, *a.shape) for a in args],
            held(BF16, 4 * width, width), held(BF16, width, width), held(BF16, width, width),
            held(BF16, tiles, width, 128),
            held(F32, tiles, width, 128), held(F32, tiles, width, 128), held(F32, tiles, width, 128),
            held(F32, 2, halves, width * high, 128),
            near_held(team, halves, 2, each * high, 128), near_held(team, halves, 2, each * high, 128),
            held(BF16, ndev, 2, max(far, 1) * tiles, 128), held(BF16, ndev, 2, max(far, 1) * tiles, 128),
            held(BF16, max(each, 1), total, side), held(BF16, max(each, 1), total, side),
            held(BF16, max(far, 1), total, total), held(BF16, max(far, 1), total, total),
            near_held(ndev, halves, each * high, 128), near_held(ndev, halves, each * high, 128),
            held(BF16, ndev, max(far, 1) * tiles, 128), held(BF16, ndev, max(far, 1) * tiles, 128),
            held(F32, width * high, 128),
            held(BF16, ncol, per, cols_dev, width),
            held(BF16, per, total, width),
            held(BF16, per, total, 2 * width),
            held(BF16, per, halves, total // halves, width),
            held(F32, per, halves, total // halves, width),
            held(F32, heads * high, 128),
            held(BF16, 2, halves, nrow, ncol // 2, heads * high, 128),
            held(F32, halves, heads, total // halves, total),
            held(BF16, halves, per, total // halves, width),
            held(BF16, halves, per, total // halves, width),
            sem(6), sem(halves), sem(), sem(max(parts, 1)), sem(), sem(max(parts, 1) + halves), sem(),
            sem(per // PAIR), sem(halves + ncol // 2), sem(2, halves), sem(halves + per),
        ],
        compiler_params=pltpu.CompilerParams(
            collective_id=0, has_side_effects=True, vmem_limit_bytes=40 * 1024 * 1024
        ),
    )(valid_length, *args)


def solution(mesh):
    placed = (P("row", "col", None), P(), P(), P(), P(), P(), P(), P())
    return jax.shard_map(
        per_device, mesh=mesh, in_specs=placed, out_specs=P("row", "col", None), check_vma=False
    )
```

```python
import functools

import jax
import jax.numpy as jnp
from jax import lax
from jax.experimental import pallas as pl
from jax.experimental.pallas import tpu as pltpu
from jax.sharding import PartitionSpec as P

MESH = pl.DeviceIdType.MESH
F32 = jnp.float32
BF16 = jnp.bfloat16
scope = jax.named_scope
PAIR = 2


def norm(values, axis):
    center = values - jnp.mean(values, axis=axis, keepdims=True)
    return center * lax.rsqrt(jnp.mean(center * center, axis=axis, keepdims=True) + 1e-05)


def swap_groups(blocks, lane, group):
    count = len(blocks)
    width = count * group
    out = []
    for b in range(count):
        total = None
        for a in range(count):
            shift = (group * (a - b)) % width
            moved = blocks[a] if shift == 0 else pltpu.roll(blocks[a], shift, 1)
            total = moved if total is None else jnp.where(lane == a, moved, total)
        out.append(total)
    return out


def arrived(ref, sem):
    pltpu.make_async_copy(ref, ref, sem).wait()


def kernel(
    dims,
    valid_h, pair_h, tri_in_h, tri_gate_h, tri_out_h, att_in_h, bias_w_h, att_out_h,
    out_ref,
    valid_ref, pair_ref, tri_in_ref, tri_gate_ref, tri_out_ref, att_in_ref, bias_w_ref, att_out_ref,
    tri_in_s, tri_gate_t, tri_out_s, normed_s, pair_s, middle_s, gate_t, edge_f,
    near_send, near_recv, far_send, far_recv, near_left, near_right, far_left, far_right,
    near_psend, near_precv, far_psend, far_precv, prod_f,
    mid_send, mid_recv, kv_s, query_s, gate_s,
    bias_f, bias_recv, bias_full, gated_s, gated_recv,
    sem_in, sem_pair, sent, recv_n, recv_f, recv_pn, recv_pf, recv_m, recv_z, recv_b, recv_g,
):
    nrow, ncol, rows_dev, cols_dev, width, heads, far, near, parts, halves = dims
    ndev = nrow * ncol
    total = ncol * cols_dev
    group = 128 // cols_dev
    tiles = rows_dev // group
    each = near // parts if parts else 0
    side_cols = ncol // 2
    team = nrow * side_cols
    per = rows_dev // ncol
    span = tiles // per
    high = tiles // halves
    nz = ncol // 2
    head_size = width // heads
    my_row, my_col = lax.axis_index("row"), lax.axis_index("col")
    me = my_row * ncol + my_col
    core, my_z = lax.rem(my_col, 2), my_col // 2
    my_side, my_rank = my_col // side_cols, my_row * side_cols + lax.rem(my_col, side_cols)

    held = (tri_in_ref, tri_gate_ref, tri_out_ref, att_in_ref, bias_w_ref, att_out_ref, valid_ref)
    given = (tri_in_h, tri_gate_h, tri_out_h, att_in_h, bias_w_h, att_out_h, valid_h)
    loads = [pltpu.make_async_copy(g, v, sem_in.at[k]) for k, (g, v) in enumerate(zip(given, held))]
    loads[0].start()
    loads[6].start()
    for hh in range(halves):
        for g in range(group):
            some = pl.ds(g * tiles + hh * high, high)
            pltpu.make_async_copy(pair_h.at[some], pair_ref.at[some], sem_pair.at[hh]).start()
    for k in (1, 2, 4, 3, 5):
        loads[k].start()

    def other(step):
        peer = lax.rem(me + step, ndev)
        return peer, (peer // ncol, lax.rem(peer, ncol))

    def loop(count, act):
        def run(step, carry):
            act(step)
            return carry

        lax.fori_loop(1, count, run, 0)

    with scope("signal"):
        barrier = pltpu.get_barrier_semaphore()
        for r in range(nrow):
            for c in range(ncol):
                pl.semaphore_signal(barrier, inc=1, device_id=(r, c), device_id_type=MESH)
    with scope("inputs"):
        loads[0].wait()
        loads[6].wait()
        tri_in_s[...] = jnp.transpose(tri_in_ref[...].astype(F32)).astype(BF16)
    valid = valid_ref[...]

    lanes = lax.broadcasted_iota(jnp.int32, (1, 128), 1)
    lane_col = my_col * cols_dev + lanes % cols_dev
    lane_row = my_row * rows_dev + (lanes // cols_dev) * tiles

    def edges(hh):
        arrived(pair_ref.at[pl.ds(0, group * high)], sem_pair.at[hh])
        for tt in range(high):
            t = hh * high + tt
            rows = jnp.concatenate([pair_ref[g * tiles + t] for g in range(group)], axis=0)
            rows = jnp.transpose(rows)
            pair_s[t] = rows
            normed = norm(rows, 0).astype(BF16)
            normed_s[t] = normed
            keep = jnp.where((lane_row + t < valid) & (lane_col < valid), 1.0, 0.0)
            for side in range(2):
                proj = jnp.dot(
                    tri_in_s[2 * side * width : 2 * (side + 1) * width, :], normed, preferred_element_type=F32
                )
                edge_f[side, hh, pl.ds(tt, width, stride=high), :] = (
                    jax.nn.sigmoid(proj[:width]) * proj[width:] * keep
                )

    def near_channel(k, rank):
        return far * ndev + k * team + rank

    def near_pack(part, hh):
        for rank in range(team):
            for side in range(2):
                for k in range(each):
                    at = near_channel(part * each + k, rank) * high
                    near_send[part, rank, hh, side, k * high : (k + 1) * high] = edge_f[
                        side, hh, at : at + high, :
                    ].astype(BF16)

    def far_pack():
        for d in range(ndev):
            for side in range(2):
                for f in range(far):
                    for hh in range(halves):
                        at = (f * ndev + d) * high
                        to = (f * halves + hh) * high
                        far_send[d, side, to : to + high] = edge_f[side, hh, at : at + high, :].astype(BF16)

    def remote(src, dst, recv, where):
        return pltpu.make_async_remote_copy(
            src_ref=src, dst_ref=dst, send_sem=sent, recv_sem=recv, device_id=where, device_id_type=MESH
        )

    def near_copy(part, hh, step):
        peer = lax.rem(my_rank + step, team)
        some = pl.ds(0, halves) if hh is None else pl.ds(hh, 1)
        return remote(
            near_send.at[part, peer, some], near_recv.at[part, my_rank, some],
            recv_n.at[part],
            (peer // side_cols, my_side * side_cols + lax.rem(peer, side_cols)),
        )

    def far_copy(step):
        peer, where = other(step)
        return remote(far_send.at[peer], far_recv.at[me], recv_f, where)

    def near_start(part, hh):
        with scope("near_start"):
            loop(team, lambda step: near_copy(part, hh, step).start())

    for hh in range(halves):
        with scope("edges"):
            edges(hh)
        if hh == 0:
            with scope("barrier"):
                pl.semaphore_wait(barrier, ndev)
        if parts:
            near_pack(0, hh)
            near_start(0, hh)
    if far:
        with scope("far_start"):
            far_pack()
            loop(ndev, lambda step: far_copy(step).start())
            far_recv[me] = far_send[me]
    for part in range(parts):
        for hh in range(halves):
            if part:
                near_pack(part, hh)
        near_recv[part, my_rank] = near_send[part, my_rank]
    for part in range(1, parts):
        near_start(part, None)
    with scope("gate"):
        for k in (1, 2, 4, 3, 5):
            loads[k].wait()
        tri_out_s[...] = jnp.transpose(tri_out_ref[...].astype(F32)).astype(BF16)
        tri_gate_t[...] = jnp.transpose(tri_gate_ref[...].astype(F32)).astype(BF16)
        for t in range(tiles):
            gate_t[t] = jax.nn.sigmoid(
                jnp.dot(tri_gate_t[...], normed_s[t], preferred_element_type=F32)
            )
    others = pl.ds(0, ndev - 1)
    chunks = [(i, 1) for i in range(per)]
    ready = per // halves
    waiting = []
    last = halves - 1
    team_others = pl.ds(0, team - 1)

    lane = lax.broadcasted_iota(jnp.int32, (tiles, 128), 1) // cols_dev

    def spread(load, columns, operand):
        for r in range(nrow):
            for half in range(columns // group):
                blocks = [load(r * columns + half * group + a) for a in range(group)]
                for b, piece in enumerate(swap_groups(blocks, lane, cols_dev)):
                    operand[
                        pl.ds(r * rows_dev + b * tiles, tiles), pl.ds(half * 128, 128)
                    ] = piece.astype(BF16)

    def multiply(left, right, put):
        products = lax.dot_general(left, right, (((1,), (1,)), ((), ())), preferred_element_type=F32)
        for r in range(nrow):
            for half in range(ncol // group):
                blocks = [
                    products[
                        r * rows_dev + a * tiles : r * rows_dev + (a + 1) * tiles,
                        half * 128 : (half + 1) * 128,
                    ]
                    for a in range(group)
                ]
                for b, piece in enumerate(swap_groups(blocks, lane, cols_dev)):
                    for hh in range(halves):
                        put(r * ncol + half * group + b, hh, piece[hh * high : (hh + 1) * high].astype(BF16))

    def near_pcopy(part, hh, step):
        peer, where = other(step)
        some = pl.ds(0, halves) if hh is None else pl.ds(hh, 1)
        return remote(
            near_psend.at[part, peer, some], near_precv.at[part, me, some],
            recv_pn.at[part + (hh or 0)], where,
        )

    def far_pcopy(step):
        peer, where = other(step)
        return remote(far_psend.at[peer], far_precv.at[me], recv_pf, where)

    def near_products(part):
        with scope("near_wait"):
            arrived(near_recv.at[part, team_others], recv_n.at[part])
        with scope("near_products"):
            for k in range(each):
                for side, operand in ((0, near_left), (1, near_right)):
                    spread(
                        lambda d: jnp.concatenate(
                            [
                                near_recv[part, d, hh, side, k * high : (k + 1) * high].astype(F32)
                                for hh in range(halves)
                            ],
                            axis=0,
                        ),
                        side_cols, operand.at[k],
                    )

                def put(d, hh, piece):
                    near_psend[part, d, hh, k * high : (k + 1) * high] = piece

                multiply(near_left[k], near_right[k], put)
        with scope("near_psend"):
            for hh in range(halves) if part == parts - 1 else (None,):
                loop(ndev, lambda step: near_pcopy(part, hh, step).start())
            near_precv[part, me] = near_psend[part, me]

    def far_products():
        with scope("far_wait"):
            arrived(far_recv.at[others], recv_f)
        with scope("far_products"):
            for f in range(far):
                for side, operand in ((0, far_left), (1, far_right)):
                    spread(
                        lambda d: far_recv[d, side, f * tiles : (f + 1) * tiles].astype(F32), ncol, operand.at[f]
                    )

                def put(d, hh, piece):
                    at = (f * halves + hh) * high
                    far_psend[d, at : at + high] = piece

                multiply(far_left[f], far_right[f], put)
        with scope("far_psend"):
            loop(ndev, lambda step: far_pcopy(step).start())
            far_precv[me] = far_psend[me]

    for part in range(parts):
        if part == 1 and far:
            far_products()
        near_products(part)
    if parts < 2:
        far_products()

    def strip(peer):
        return pl.ds(pl.multiple_of(peer * cols_dev, cols_dev), cols_dev)

    def send_rows(chunk, steps):
        first, count = chunks[chunk]
        some = pl.ds(first, count)
        for step in steps:
            peer = lax.rem(my_col + step, ncol)
            remote(
                mid_send.at[peer, some], mid_recv.at[some, strip(my_col), :],
                recv_m.at[first // PAIR], (my_row, peer),
            ).start()

    def keep_rows(chunk):
        first, count = chunks[chunk]
        for i in range(first, first + count):
            mid_recv[i, strip(my_col), :] = mid_send[my_col, i]

    def bias_block(hh, z):
        block = bias_recv.at[core, hh, my_row, z]
        for step in range(1, nrow):
            peer = lax.rem(my_row + step, nrow)
            remote(block, block, recv_b.at[0, hh], (peer, my_col)).start()

    def bias_z(hh):
        mine = bias_recv.at[core, hh, my_row, my_z]
        for step in range(1, nz):
            peer = lax.rem(my_z + step, nz)
            remote(mine, mine, recv_z.at[hh if hh < last else last + my_z], (my_row, 2 * peer + core)).start()
        if hh == last:
            bias_block(hh, my_z)

    def bias_row(hh):
        if hh < last:
            arrived(bias_recv.at[0, hh, 0, pl.ds(0, nz - 1)], recv_z.at[hh])
            bias_block(hh, slice(None))
            return
        turn = 1 - 2 * (my_z // (nz // 2))
        for step in range(1, nz):
            z = lax.rem(my_z + turn * step + nz, nz)
            arrived(bias_recv.at[0, hh, 0, 0], recv_z.at[last + z])
            bias_block(hh, z)

    def bias_hand(hh):
        mine = bias_recv.at[core, hh]
        return remote(mine, mine, recv_b.at[1, hh], (my_row, my_col + 1 - 2 * core))

    def bias_core(hh):
        arrived(bias_recv.at[0, hh, pl.ds(0, nrow - 1)], recv_b.at[0, hh])
        bias_hand(hh).start()

    for hh in range(halves):
        with scope("waitp"):
            if hh == 0:
                if far:
                    arrived(far_precv.at[others], recv_pf)
                for part in range(parts - 1):
                    arrived(near_precv.at[part, others], recv_pn.at[part])
            if parts:
                arrived(near_precv.at[parts - 1, others, hh], recv_pn.at[parts - 1 + hh])
        with scope("unpack"):
            for f in range(far):
                for d in range(ndev):
                    at = (f * ndev + d) * high
                    of = (f * halves + hh) * high
                    prod_f[at : at + high, :] = far_precv[d, of : of + high].astype(F32)
            for part in range(parts):
                for rank in range(team):
                    one = (rank // side_cols) * ncol + rank % side_cols
                    for k in range(each):
                        at = near_channel(part * each + k, rank) * high
                        of = slice(k * high, (k + 1) * high)
                        prod_f[at : at + high, :] = near_precv[part, one, hh, of].astype(F32) + near_precv[
                            part, one + side_cols, hh, of
                        ].astype(F32)
        with scope("middle"):
            for tt in range(high):
                t = hh * high + tt
                prods = norm(prod_f[pl.ds(tt, width, stride=high), :], 0).astype(BF16)
                update = jnp.dot(tri_out_s[...], prods, preferred_element_type=F32)
                middle = pair_s[t] + gate_t[t] * update
                middle_s[t] = middle
                normed_mid = norm(middle, 0)
                own = jnp.dot(bias_w_ref[...], normed_mid.astype(BF16), preferred_element_type=F32)
                for h in range(heads):
                    bias_f[pl.ds(h * high + tt, 1), :] = own[h : h + 1]
                normed_mid = jnp.transpose(normed_mid).astype(BF16)
                for g in range(group):
                    mid_send[g * span + t % span, t // span] = normed_mid[g * cols_dev : (g + 1) * cols_dev]
        with scope("bias_z"):
            bias_recv[core, hh, my_row, my_z] = bias_f[...].astype(BF16)
            bias_z(hh)
        with scope("send_rows"):
            fresh = [chunk for chunk, (first, _) in enumerate(chunks) if first // ready == hh]
            held = max(1, len(fresh) // 4) if hh < halves - 1 else 0
            for chunk in waiting + fresh[: len(fresh) - held]:
                send_rows(chunk, range(1, ncol))
                keep_rows(chunk)
            waiting = fresh[len(fresh) - held :]

    def take(i):
        if i % PAIR == 0:
            arrived(mid_recv.at[pl.ds(i, PAIR), pl.ds(0, (ncol - 1) * cols_dev), :], recv_m.at[i // PAIR])

    tokens = lax.broadcasted_iota(jnp.int32, (1, total), 1)
    mask = jnp.where(tokens < valid, 0.0, -1000000000.0)
    narrow = lax.broadcasted_iota(jnp.int32, (high, 128), 1) // cols_dev

    def assemble(hh):
        arrived(bias_recv.at[0, hh], recv_b.at[1, hh])
        for h in range(heads):
            for r in range(nrow):
                for half in range(ncol // group):
                    blocks = []
                    for a in range(group):
                        c = half * group + a
                        blocks.append(
                            bias_recv[c % 2, hh, r, c // 2, h * high : (h + 1) * high, :].astype(F32)
                        )
                    for b, piece in enumerate(swap_groups(blocks, narrow, cols_dev)):
                        bias_full[
                            hh, h, pl.ds((r * group + b) * high, high), pl.ds(half * 128, 128)
                        ] = piece + mask[:, half * 128 : (half + 1) * 128]

    def project(i):
        with scope("take"):
            take(i)
        with scope("project"):
            proj = jnp.dot(mid_recv[i], att_in_ref[...], preferred_element_type=F32)
            kv_s[i] = proj[:, width : 3 * width].astype(BF16)
            query = proj[:, :width] * head_size ** (-0.5)
            gate = jax.nn.sigmoid(proj[:, 3 * width :])
            for hh in range(halves):
                pick = lambda x: jnp.concatenate(
                    [x[at : at + high] for at in range(hh * high, total, tiles)], axis=0
                )
                query_s[i, hh] = pick(query).astype(BF16)
                gate_s[i, hh] = pick(gate)

    with scope("bias_row"):
        bias_row(0)
    with scope("keep_middle"):
        for t in range(tiles):
            middle = jnp.transpose(middle_s[t])
            for g in range(group):
                out_ref[g * tiles + t] = middle[g * cols_dev : (g + 1) * cols_dev]
    with scope("bias_core"):
        bias_core(0)

    block = min(128, total // halves)
    own_cols = cols_dev // halves
    head = lax.broadcasted_iota(jnp.int32, (block, width), 1) // head_size

    def share_cols(peer):
        return pl.ds(pl.multiple_of(peer * own_cols, own_cols), own_cols)

    def send_home(hh, first, count):
        some = pl.ds(first, count)
        for step in range(1, ncol):
            peer = lax.rem(my_col + step, ncol)
            remote(
                gated_s.at[hh, some, share_cols(peer), :], gated_recv.at[hh, some, share_cols(my_col), :],
                recv_g.at[hh if hh < last else last + first // PAIR], (my_row, peer),
            ).start()

    def attend(hh, i):
        keys = kv_s[i, :, :width]
        values = jnp.concatenate([kv_s[i, :, width:], jnp.ones((total, width), BF16)], axis=1)
        for first in range(0, total // halves, block):
            query = query_s[i, hh, first : first + block, :]
            top = jnp.zeros((block, width), F32)
            bottom = jnp.ones((block, width), F32)
            for h in range(heads):
                scores = lax.dot_general(
                    jnp.where(head == h, query, jnp.zeros_like(query)), keys,
                    (((1,), (1,)), ((), ())), preferred_element_type=F32,
                )
                scores = scores + bias_full[hh, h, first : first + block, :]
                expo = jnp.exp(scores - jnp.max(scores, axis=1, keepdims=True)).astype(BF16)
                both = jnp.dot(expo, values, preferred_element_type=F32)
                top = jnp.where(head == h, both[:, :width], top)
                bottom = jnp.where(head == h, both[:, width:], bottom)
            gated_s[hh, i, first : first + block, :] = (
                gate_s[i, hh, first : first + block, :] * top / bottom
            ).astype(BF16)

    def attend_batch(hh, first):
        for k in range(ready):
            attend(hh, first + k)
        size = ready if hh < last else PAIR
        for k in range(0, ready, size):
            send_home(hh, first + k, size)
        for k in range(ready):
            gated_recv[hh, first + k, share_cols(my_col), :] = gated_s[hh, first + k, share_cols(my_col), :]

    def run(first, last, act):
        def body(i, carry):
            act(i)
            return carry

        lax.fori_loop(first, last, body, 0)

    for i in range(min(PAIR, ready)):
        project(i)
    with scope("bias_row"):
        for hh in range(1, halves):
            bias_row(hh)
    for i in range(PAIR, ready):
        project(i)
    with scope("assemble"):
        assemble(0)
    with scope("attend"):
        attend_batch(0, 0)
    with scope("bias_core"):
        for hh in range(1, halves):
            bias_core(hh)
    for first in range(ready, per, ready):
        for i in range(first, first + ready):
            project(i)
        with scope("attend"):
            attend_batch(0, first)
    for hh in range(1, halves):
        with scope("assemble"):
            assemble(hh)
        with scope("attend"):
            run(0, per // ready, lambda k: attend_batch(hh, k * ready))

    def finish(hh, i):
        if hh == last:
            if i % PAIR == 0:
                with scope("waitg"):
                    arrived(
                        gated_recv.at[hh, pl.ds(i, PAIR), pl.ds(0, (ncol - 1) * own_cols), :],
                        recv_g.at[last + i // PAIR],
                    )
        added = jnp.dot(gated_recv[hh, i], att_out_ref[...], preferred_element_type=F32)
        for q in range(ncol):
            row = (q // span) * tiles + i * span + q % span
            for m in range(own_cols // high):
                at = q * own_cols + m * high
                out_ref[row, m * tiles + hh * high : m * tiles + (hh + 1) * high] += added[at : at + high]

    with scope("finish"):
        for hh in range(halves):
            if hh < last:
                arrived(gated_recv.at[hh, :, pl.ds(0, (ncol - 1) * own_cols), :], recv_g.at[hh])
            for i in range(per):
                finish(hh, i)
    with scope("drain"):
        arrived(far_recv.at[others], sent)
        arrived(far_precv.at[others], sent)
        for part in range(parts):
            arrived(near_recv.at[part, team_others], sent)
            for hh in range(halves):
                arrived(near_precv.at[part, others, hh], sent)
        arrived(mid_recv.at[:, pl.ds(0, (ncol - 1) * cols_dev), :], sent)
        for hh in range(halves):
            arrived(gated_recv.at[hh, :, pl.ds(0, (ncol - 1) * own_cols), :], sent)
            arrived(bias_recv.at[0, hh, 0, pl.ds(0, nz - 1)], sent)
            arrived(bias_recv.at[0, hh, pl.ds(0, nrow - 1)], sent)
            arrived(bias_recv.at[0, hh], sent)


def per_device(pair, valid_length, tri_in, tri_gate, tri_out, att_in, att_bias, att_out):
    rows_dev, cols_dev, width = pair.shape
    heads = att_bias.shape[1]
    nrow, ncol = lax.axis_size("row"), lax.axis_size("col")
    ndev = nrow * ncol
    total = ncol * cols_dev
    tiles = rows_dev // (128 // cols_dev)
    chans = width // ndev
    far = max(1, chans // 4)
    near = 2 * (chans - far)
    parts = 2 if near else 0
    each = near // 2
    team = ndev // 2
    side = ncol // 2 * cols_dev
    per = rows_dev // ncol
    halves = 2 if tiles % 16 == 0 and (tiles // 2) % per == 0 else 1
    high = tiles // halves
    hbm = pl.BlockSpec(memory_space=pltpu.HBM)
    held = lambda dtype, *shape: pltpu.VMEM(shape, dtype)
    sem = lambda *shape: pltpu.SemaphoreType.DMA(shape) if shape else pltpu.SemaphoreType.DMA
    near_held = lambda *shape: held(BF16, *((parts,) + shape if parts else (1, 8, 128)))
    bias_w = att_bias.T
    args = [pltpu.with_memory_space_constraint(a, pltpu.HBM) for a in (pair, tri_in, tri_gate, tri_out, att_in, bias_w, att_out)]
    return pl.pallas_call(
        functools.partial(kernel, (nrow, ncol, rows_dev, cols_dev, width, heads, far, near, parts, halves)),
        out_shape=jax.ShapeDtypeStruct((rows_dev, cols_dev, width), F32),
        in_specs=[pl.BlockSpec(memory_space=pl.ANY)] + [hbm] * 7,
        out_specs=pl.BlockSpec(memory_space=pltpu.VMEM),
        scratch_shapes=[
            held(jnp.int32, 1, 1),
            *[held(a.dtype, *a.shape) for a in args],
            held(BF16, 4 * width, width), held(BF16, width, width), held(BF16, width, width),
            held(BF16, tiles, width, 128),
            held(F32, tiles, width, 128), held(F32, tiles, width, 128), held(F32, tiles, width, 128),
            held(F32, 2, halves, width * high, 128),
            near_held(team, halves, 2, each * high, 128), near_held(team, halves, 2, each * high, 128),
            held(BF16, ndev, 2, max(far, 1) * tiles, 128), held(BF16, ndev, 2, max(far, 1) * tiles, 128),
            held(BF16, max(each, 1), total, side), held(BF16, max(each, 1), total, side),
            held(BF16, max(far, 1), total, total), held(BF16, max(far, 1), total, total),
            near_held(ndev, halves, each * high, 128), near_held(ndev, halves, each * high, 128),
            held(BF16, ndev, max(far, 1) * tiles, 128), held(BF16, ndev, max(far, 1) * tiles, 128),
            held(F32, width * high, 128),
            held(BF16, ncol, per, cols_dev, width),
            held(BF16, per, total, width),
            held(BF16, per, total, 2 * width),
            held(BF16, per, halves, total // halves, width),
            held(F32, per, halves, total // halves, width),
            held(F32, heads * high, 128),
            held(BF16, 2, halves, nrow, ncol // 2, heads * high, 128),
            held(F32, halves, heads, total // halves, total),
            held(BF16, halves, per, total // halves, width),
            held(BF16, halves, per, total // halves, width),
            sem(7), sem(halves), sem(), sem(max(parts, 1)), sem(), sem(max(parts, 1) + halves), sem(),
            sem(per // PAIR), sem(halves + ncol // 2), sem(2, halves), sem(halves + per // PAIR),
        ],
        compiler_params=pltpu.CompilerParams(
            collective_id=0, has_side_effects=True, vmem_limit_bytes=40 * 1024 * 1024
        ),
    )(valid_length.reshape(1, 1), *args)


def solution(mesh):
    placed = (P("row", "col", None), P(), P(), P(), P(), P(), P(), P())
    return jax.shard_map(
        per_device, mesh=mesh, in_specs=placed, out_specs=P("row", "col", None), check_vma=False
    )
```
